128 devices in a mesh: doc: 8 (over z_lo, y), ctx: 16 (over x, z_hi, core).
Axes of the slice: x: 4, y: 4, z: 4 (z_hi: 2, z_lo: 2; z = z_hi * 2 + z_lo), core: 2. Of those that a mesh axis runs over, the one named last changes fastest.
Arguments:
- summary_cache: bfloat16 [8, 64, 512, 2048], P(None, 'doc', None, 'ctx'), may hold values from -4 to 4
- queries: bfloat16 [8, 4096, 4096], P('doc', 'ctx'), may hold values from -100 to 100
- section_counts: int32 [64], replicated, may hold values from 1 to 2
- summary_blocks: int32 [64, 2], replicated, may hold values from 1 to 2
Outputs:
- attended: bfloat16 [8, 4096, 4096], P('doc', 'ctx')
- relayed: bfloat16 [8, 8, 4096, 2048], P(None, 'doc', 'ctx')
The draws below stay inside these ranges and needn't reach their ends.
All inputs are finite; a program needn't handle non-finite values.
Results may differ from the reference program's by a relative error of at most 0.0045.
Values may be sent and summed in bfloat16 or wider, within the bound.
A program may use at most 192 MiB of HBM per device.

```python
import math
import jax
import jax.numpy as jnp
from jax import lax

QH = 32
KVH = 8
HD = 128
LAYERS = 8
BLOCK = 128
SUMBLK = 2
SECTIONS = 2
GROUP = 4
FEAT = 2048
SUMLEN = 256
SEQD = 512
GROUPS = 8
DOCS = 64
GSEQ = 4096


def draw_summary_cache(key, part):
    array_shape = (LAYERS, DOCS, SEQD, FEAT)
    base_key = jax.random.fold_in(key, 3)
    values = jnp.clip(jax.random.normal(base_key, array_shape, jnp.float32), -4.0, 4.0)
    return values.astype(jnp.bfloat16)


def draw_queries(key, part):
    array_shape = (GROUPS, GSEQ, QH * HD)
    base_key = jax.random.fold_in(key, 5)
    values = jnp.clip(jax.random.normal(base_key, array_shape, jnp.float32), -4.0, 4.0)
    return values.astype(jnp.bfloat16)


def with_ends(values, key, least, largest):
    longest = values.shape.index(max(values.shape))
    spots = []
    for shift in (0, 1):
        where = [jax.random.randint(jax.random.fold_in(key, axis), (), 0, length) for axis, length in enumerate(values.shape)]
        where[longest] = (where[longest] + shift) % values.shape[longest]
        spots.append(tuple(where))
    return values.at[spots[0]].set(least).at[spots[1]].set(largest)


def setup_inputs(seed: int = 0) -> dict:
    arg_keys = jax.random.split(jax.random.key(seed), 5)
    summary_cache = draw_summary_cache(jax.random.fold_in(arg_keys[4], 71), 0)
    queries = draw_queries(jax.random.fold_in(arg_keys[4], 71), 0)
    section_counts = with_ends(jax.random.randint(arg_keys[2], (DOCS,), 1, SECTIONS + 1), jax.random.fold_in(arg_keys[2], 1), 1, SECTIONS).astype(jnp.int32)
    summary_blocks = with_ends(jax.random.randint(arg_keys[3], (DOCS, SECTIONS), 1, SUMBLK + 1), jax.random.fold_in(arg_keys[3], 1), 1, SUMBLK).astype(jnp.int32)
    return dict(summary_cache=summary_cache, queries=queries, section_counts=section_counts, summary_blocks=summary_blocks)


NEGATIVE = -1e+30

def attend_group(operands):
    query_rows, key_rows, validity = operands
    block_rows = min(GSEQ, 512)
    pieces = []
    for offset in range(0, GSEQ, block_rows):
        key_end = offset + block_rows
        grouped = query_rows[offset:key_end].astype(jnp.float32).reshape(block_rows, KVH, GROUP, HD)
        key_heads = key_rows[:key_end, :KVH * HD].astype(jnp.float32).reshape(key_end, KVH, HD)
        value_heads = key_rows[:key_end, KVH * HD:].astype(jnp.float32).reshape(key_end, KVH, HD)
        scores = jnp.einsum('pkgd,skd->kgps', grouped, key_heads) * (1.0 / math.sqrt(HD))
        key_positions = jnp.arange(key_end)
        query_positions = offset + jnp.arange(block_rows)
        allowed = validity[None, :key_end] & (key_positions[None, :] <= query_positions[:, None])
        masked = jnp.where(allowed, scores, NEGATIVE)
        row_maximum = lax.optimization_barrier(jnp.max(masked, axis=-1, keepdims=True))
        weights = jnp.where(allowed, jnp.exp(masked - row_maximum), 0.0)
        denominator = lax.optimization_barrier(jnp.sum(weights, axis=-1))
        rounded = lax.optimization_barrier(weights.astype(jnp.bfloat16)).astype(jnp.float32)
        accumulated = jnp.einsum('kgps,skd->kgpd', rounded, value_heads)
        result = accumulated / denominator[..., None]
        pieces.append(jnp.transpose(result, (2, 0, 1, 3)).reshape(block_rows, QH * HD))
    return jnp.concatenate(pieces, axis=0).astype(jnp.bfloat16)

def reference(summary_cache, queries, section_counts, summary_blocks):
    relayed = jnp.transpose(summary_cache.reshape(LAYERS, GROUPS, GROUPS, SEQD, FEAT), (0, 2, 1, 3, 4)).reshape(LAYERS, GROUPS, GSEQ, FEAT)
    counts_table = jnp.transpose(section_counts.reshape(GROUPS, GROUPS), (1, 0))
    blocks_table = jnp.transpose(summary_blocks.reshape(GROUPS, GROUPS, SECTIONS), (1, 0, 2))
    live_section = jnp.arange(SECTIONS)[None, None, :] < counts_table[:, :, None]
    live_slot = jnp.arange(SUMLEN)[None, None, None, :] < BLOCK * blocks_table[:, :, :, None]
    validity = (live_section[..., None] & live_slot).reshape(GROUPS, GSEQ)
    attended = lax.map(attend_group, (queries, relayed[0], validity))
    return (attended, relayed)
```

```python
import functools
import math

import jax
import jax.numpy as jnp
from jax import lax
from jax.experimental import pallas as pl
from jax.experimental.pallas import tpu as pltpu
from jax.sharding import PartitionSpec as P

QH = 32
KVH = 8
HD = 128
BLOCK = 128
SECTIONS = 2
GROUP = 4
SUMLEN = 256
SEQD = 512
LAYERS = 8
GSEQ = 4096
CHUNKS = 16
NEGATIVE = -1e30
MESH = pl.DeviceIdType.MESH
SCALE = (1.0 / math.sqrt(HD)) * math.log2(math.e)


def place(x, y, z, core):
    return (lax.rem(z, 2) * 4 + y, x * 4 + (z // 2) * 2 + core)


def relay_kernel(cache, out, keys, ybuf, z0, zbuf, ysend, yrecv, yown, zsend, zrecv, xsend, xrecv, xown, gsend, grecv, gown, fsend, frecv, oown):
    d = lax.axis_index("doc")
    c = lax.axis_index("ctx")
    zl, y = d // 4, lax.rem(d, 4)
    x, zh, core = c // 4, lax.rem(c // 2, 2), lax.rem(c, 2)
    z = zh * 2 + zl
    chunk = zh * 2 + core
    doc_here = x * 2 + zh
    sibling = place(x, y, z, 1 - core)

    def remote(src, dst, ssem, rsem, dev):
        return pltpu.make_async_remote_copy(src, dst, ssem, rsem, device_id=dev, device_id_type=MESH)

    def y_copy(layer, step):
        to = lax.rem(y + step, 4)
        return remote(cache.at[layer, :, to], ybuf.at[layer, y], ysend.at[layer, step - 1], yrecv.at[layer, step - 1], place(x, to, z, core))

    def y_keep(layer):
        return pltpu.make_async_copy(cache.at[layer, :, y], ybuf.at[layer, y], yown.at[layer])

    @pl.loop(0, LAYERS)
    def _(layer):
        for step in (1, 3, 2):
            y_copy(layer, step).start()
        y_keep(layer).start()

    def wait_y(layer):
        for step in (1, 2, 3):
            y_copy(layer, step).wait_recv()
        y_keep(layer).wait()

    def g_z(step, flip):
        to_z, to_core = lax.rem(z + step, 4), lax.rem(core + flip, 2)
        src = ybuf.at[0, :, lax.rem(to_z, 2), to_core]
        dst = z0.at[chunk, pl.ds(zl * 4, 4)]
        r = step * 2 + flip
        if r == 0:
            return pltpu.make_async_copy(src, dst, zrecv.at[0, 0])
        return remote(src, dst, zsend.at[0, r], zrecv.at[0, r], place(x, y, to_z, to_core))

    wait_y(0)
    for step, flip in ((1, 0), (1, 1), (3, 0), (3, 1), (2, 0), (2, 1), (0, 1), (0, 0)):
        g_z(step, flip).start()
    for r in range(8):
        if r == 0:
            g_z(0, 0).wait()
        else:
            g_z(r // 2, r % 2).wait_recv()

    def g_x(piece, step, to, docs):
        src = z0.at[piece, pl.ds(0, docs)]
        dst = keys.at[x * 4 + piece, pl.ds(0, docs), core]
        return remote(src, dst, gsend.at[piece, step - 1], grecv.at[piece, step - 1], place(to, y, z, core))

    for piece in range(4):
        for step in (1, 3, 2):
            to = lax.rem(x + step, 4)
            for v in range(4):
                @pl.when(to == v)
                def _():
                    g_x(piece, step, to, 2 * (v + 1)).start()

    def g_own(piece, docs):
        return pltpu.make_async_copy(z0.at[piece, pl.ds(0, docs)], keys.at[x * 4 + piece, pl.ds(0, docs), core], gown.at[piece])

    def g_f(piece, step, docs):
        frm = lax.rem(x - step + 4, 4)
        dst = keys.at[frm * 4 + piece, pl.ds(0, docs), core]
        src = z0.at[piece, pl.ds(0, docs)] if step == 0 else dst
        return remote(src, dst, fsend.at[piece, step], frecv.at[piece, step], sibling)

    def own_row(piece, step):
        frm = lax.rem(x - step + 4, 4)
        cols = pl.ds(pl.multiple_of((frm * 4 + piece) * HD, HD), HD)
        src = z0.at[piece, doc_here] if step == 0 else keys.at[frm * 4 + piece, doc_here, core]
        return pltpu.make_async_copy(src, out.at[0, :, cols], oown.at[piece, step])

    def each_x(body):
        for v in range(4):
            @pl.when(x == v)
            def _():
                body(2 * (v + 1))

    def first(docs):
        for piece in range(4):
            g_own(piece, docs).start()
            g_f(piece, 0, docs).start()

    each_x(first)
    for piece in range(4):
        own_row(piece, 0).start()

    def z_copy(layer, step, flip):
        to_z, to_core = lax.rem(z + step, 4), lax.rem(core + flip, 2)
        r = step * 2 + flip
        src = ybuf.at[layer, pl.ds(to_z // 2, 2, 2), lax.rem(to_z, 2), to_core]
        dst = zbuf.at[layer - 1, pl.ds(zl * 2, 2), chunk]
        return src, dst, to_z, to_core, r

    def z_one(layer, step, flip, hi):
        to_z, to_core = lax.rem(z + step, 4), lax.rem(core + flip, 2)
        r = step * 2 + flip
        src = ybuf.at[layer, hi * 2 + to_z // 2, lax.rem(to_z, 2), to_core]
        dst = zbuf.at[layer - 1, zl * 2 + hi, chunk]
        if r == 0:
            return pltpu.make_async_copy(src, dst, zrecv.at[layer, hi * 8])
        return remote(src, dst, zsend.at[layer, hi * 8 + r], zrecv.at[layer, hi * 8 + r], place(x, y, to_z, to_core))

    def x_copy(layer, step, piece):
        to = lax.rem(x + step, 4)
        cols = pl.ds(pl.multiple_of((x * 4 + piece) * HD, HD), HD)
        src = zbuf.at[layer - 1, to, piece]
        dst = out.at[layer, :, cols]
        if step == 0:
            return pltpu.make_async_copy(src, dst, xown.at[layer - 1, piece])
        return remote(src, dst, xsend.at[layer - 1, step - 1, piece], xrecv.at[layer - 1, step - 1, piece], place(to, y, z, core))

    def pass_on(piece):
        def body(docs):
            for step in (1, 3, 2):
                g_x(piece, step, x, docs).wait_recv()
                g_f(piece, step, docs).start()
        each_x(body)
        for step in (1, 3, 2):
            own_row(piece, step).start()

    @pl.loop(1, LAYERS)
    def _(layer):
        wait_y(layer)
        for step, flip in ((1, 0), (1, 1), (3, 0), (3, 1), (2, 0), (2, 1), (0, 1), (0, 0)):
            for hi in range(2):
                z_one(layer, step, flip, hi).start()
        for r in range(8):
            for hi in range(2):
                if r == 0:
                    z_one(layer, 0, 0, hi).wait()
                else:
                    z_one(layer, r // 2, r % 2, hi).wait_recv()
        for step in (1, 3, 2, 0):
            for piece in range(4):
                x_copy(layer, step, piece).start()

    for piece in range(4):
        pass_on(piece)

    def drain(docs):
        for piece in range(4):
            g_own(piece, docs).wait()
            for step in range(4):
                g_f(piece, step, docs).wait()

    each_x(drain)
    for piece in range(4):
        for step in (1, 3, 2):
            to = lax.rem(x + step, 4)
            for v in range(4):
                @pl.when(to == v)
                def _():
                    g_x(piece, step, to, 2 * (v + 1)).wait_send()
        for step in range(4):
            own_row(piece, step).wait()
    for r in range(1, 8):
        g_z(r // 2, r % 2).wait_send()
    for step in (1, 2, 3):
        y_copy(0, step).wait_send()

    @pl.loop(1, LAYERS)
    def _(layer):
        for step in (1, 2, 3):
            y_copy(layer, step).wait_send()
        for r in range(1, 8):
            for hi in range(2):
                z_one(layer, r // 2, r % 2, hi).wait_send()
        for piece in range(4):
            x_copy(layer, 0, piece).wait()
            for step in (1, 2, 3):
                x_copy(layer, step, piece).wait()


def relay(cache):
    dma = pltpu.SemaphoreType.DMA
    bf = jnp.bfloat16
    anyspace = pl.BlockSpec(memory_space=pl.ANY)
    return pl.pallas_call(
        relay_kernel,
        out_shape=(
            jax.ShapeDtypeStruct((LAYERS, 256, 2048), bf),
            jax.ShapeDtypeStruct((CHUNKS, 8, 2, 256, HD), bf),
            jax.ShapeDtypeStruct((LAYERS, 4, 2, 2, 256, HD), bf),
        ),
        in_specs=[anyspace],
        out_specs=(anyspace,) * 3,
        scratch_shapes=[
            pltpu.VMEM((4, 8, 256, HD), bf),
            pltpu.VMEM((LAYERS - 1, 4, 4, 256, HD), bf),
            dma((8, 3)), dma((8, 3)), dma((8,)),
            dma((8, 16)), dma((8, 16)),
            dma((7, 3, 4)), dma((7, 3, 4)), dma((7, 4)),
            dma((4, 3)), dma((4, 3)), dma((4,)),
            dma((4, 4)), dma((4, 4)), dma((4, 4)),
        ],
        compiler_params=pltpu.CompilerParams(has_side_effects=True, vmem_limit_bytes=40 << 20),
    )(cache.reshape(LAYERS, 2, 4, 2, 256, HD))


def attend_kernel(q_ref, k_ref, v_ref, bias_ref, o_ref, m_ref, l_ref, acc_ref):
    c = lax.axis_index("ctx")
    mine = c // 2
    half = lax.rem(c, 2)
    q = jnp.concatenate([q_ref[:, g * HD : (g + 1) * HD] for g in range(GROUP)], axis=0)
    rows = q.shape[0]

    def step(doc, diagonal, first):
        k = k_ref[0, pl.ds(pl.multiple_of(doc * SEQD, SEQD), SEQD), :]
        v = v_ref[0, pl.ds(pl.multiple_of(doc * SEQD, SEQD), SEQD), :]
        s = lax.dot_general(q, k, (((1,), (1,)), ((), ())), preferred_element_type=jnp.float32)
        s = s * SCALE + bias_ref[pl.ds(doc, 1), :]
        if diagonal:
            at = lax.rem(lax.broadcasted_iota(jnp.int32, s.shape, 0), 256) + half * 256
            s = jnp.where(lax.broadcasted_iota(jnp.int32, s.shape, 1) <= at, s, NEGATIVE)
        top = m_ref[...]
        newest = jnp.maximum(top, jnp.max(s, axis=1, keepdims=True))
        w = jnp.exp2(s - newest)
        factor = jnp.exp2(top - newest)
        m_ref[...] = newest
        part = w[:, 0:128] + w[:, 128:256] + w[:, 256:384] + w[:, 384:512]
        l_ref[...] = l_ref[...] * factor + part
        acc_ref[...] = acc_ref[...] * factor + lax.dot_general(
            w.astype(jnp.bfloat16), v, (((1,), (0,)), ((), ())), preferred_element_type=jnp.float32
        )

    m_ref[...] = jnp.full(m_ref.shape, NEGATIVE, jnp.float32)
    l_ref[...] = jnp.zeros_like(l_ref)
    acc_ref[...] = jnp.zeros_like(acc_ref)

    @pl.loop(0, mine)
    def _(doc):
        step(doc, False, False)

    step(mine, True, False)
    result = (acc_ref[...] / jnp.sum(l_ref[...], axis=1, keepdims=True)).astype(jnp.bfloat16)
    for g in range(GROUP):
        o_ref[:, g * HD : (g + 1) * HD] = result[g * 256 : (g + 1) * 256]


def attention(queries, keys, bias):
    return pl.pallas_call(
        attend_kernel,
        grid=(KVH,),
        out_shape=jax.ShapeDtypeStruct((256, QH * HD), jnp.bfloat16),
        in_specs=[
            pl.BlockSpec((256, GROUP * HD), lambda k: (0, k)),
            pl.BlockSpec((1, GSEQ, HD), lambda k: (k, 0, 0)),
            pl.BlockSpec((1, GSEQ, HD), lambda k: (k + KVH, 0, 0)),
            pl.BlockSpec((8, SEQD), lambda k: (0, 0)),
        ],
        out_specs=pl.BlockSpec((256, GROUP * HD), lambda k: (0, k)),
        scratch_shapes=[
            pltpu.VMEM((GROUP * 256, 1), jnp.float32),
            pltpu.VMEM((GROUP * 256, 128), jnp.float32),
            pltpu.VMEM((GROUP * 256, HD), jnp.float32),
        ],
        compiler_params=pltpu.CompilerParams(vmem_limit_bytes=40 << 20),
    )(queries, keys, keys, bias)


def key_bias(section_counts, summary_blocks):
    chosen = (jnp.arange(8) == lax.axis_index("doc")).astype(jnp.int32)
    counts = jnp.sum(section_counts.reshape(8, 8) * chosen[None, :], axis=1)
    blocks = jnp.sum(summary_blocks.reshape(8, 8, SECTIONS) * chosen[None, :, None], axis=1)
    live_section = jnp.arange(SECTIONS)[None, :] < counts[:, None]
    live_slot = jnp.arange(SUMLEN)[None, None, :] < BLOCK * blocks[:, :, None]
    live = (live_section[:, :, None] & live_slot).reshape(8, SEQD)
    return jnp.where(live, 0.0, NEGATIVE).astype(jnp.float32)


def local(summary_cache, queries, section_counts, summary_blocks):
    bias = key_bias(section_counts, summary_blocks)
    relayed, keys, _ = relay(summary_cache)
    attended = attention(queries[0], keys.reshape(CHUNKS, GSEQ, HD), bias)
    return attended[None], relayed[:, None]


def solution(mesh):
    placed = (P(None, "doc", None, "ctx"), P("doc", "ctx", None), P(), P())
    return jax.shard_map(
        local,
        mesh=mesh,
        in_specs=placed,
        out_specs=(P("doc", "ctx", None), P(None, "doc", "ctx", None)),
        check_vma=False,
    )
```

```python
import functools
import math

import jax
import jax.numpy as jnp
from jax import lax
from jax.experimental import pallas as pl
from jax.experimental.pallas import tpu as pltpu
from jax.sharding import PartitionSpec as P

QH = 32
KVH = 8
HD = 128
BLOCK = 128
SECTIONS = 2
GROUP = 4
SUMLEN = 256
SEQD = 512
LAYERS = 8
GSEQ = 4096
CHUNKS = 16
NEGATIVE = -1e30
MESH = pl.DeviceIdType.MESH
SCALE = (1.0 / math.sqrt(HD)) * math.log2(math.e)


def place(x, y, z, core):
    return (lax.rem(z, 2) * 4 + y, x * 4 + (z // 2) * 2 + core)


def head_group(mine, half, q_ref, k_ref, v_ref, bias_ref, s_ref, m_ref, l_ref, acc_ref):
    rows = q_ref.shape[0]

    def score(doc, diagonal):
        k = k_ref[doc // 2, lax.rem(doc, 2)]
        s = lax.dot_general(q_ref[...], k, (((1,), (1,)), ((), ())), preferred_element_type=jnp.float32)
        s = s * SCALE + bias_ref[pl.ds(doc, 1), :]
        if diagonal:
            at = lax.rem(lax.broadcasted_iota(jnp.int32, s.shape, 0), 256) + half * 256
            s = jnp.where(lax.broadcasted_iota(jnp.int32, s.shape, 1) <= at, s, NEGATIVE)
        s_ref[doc] = s
        top = jnp.maximum(jnp.maximum(s[:, 0:128], s[:, 128:256]), jnp.maximum(s[:, 256:384], s[:, 384:512]))
        return top

    def weigh(doc):
        v = v_ref[doc // 2, lax.rem(doc, 2)]
        top = m_ref[...]
        w = [jnp.exp2(s_ref[doc, :, i * 128 : (i + 1) * 128] - top) for i in range(4)]
        part = (w[0] + w[1]) + (w[2] + w[3])
        pair = [jnp.concatenate([w[2 * i].astype(jnp.bfloat16), w[2 * i + 1].astype(jnp.bfloat16)], axis=1) for i in range(2)]
        summed = lax.dot_general(
            jnp.concatenate(pair, axis=1), v, (((1,), (0,)), ((), ())), preferred_element_type=jnp.float32
        )
        return part, summed

    m_ref[...] = score(mine, True)

    @pl.loop(0, mine)
    def _(doc):
        m_ref[...] = jnp.maximum(m_ref[...], score(doc, False))

    m_ref[...] = jnp.broadcast_to(jnp.max(m_ref[...], axis=1, keepdims=True), m_ref.shape)
    part, summed = weigh(mine)
    l_ref[...] = part
    acc_ref[...] = summed

    @pl.loop(0, mine)
    def _(doc):
        part, summed = weigh(doc)
        l_ref[...] += part
        acc_ref[...] += summed

    return (acc_ref[...] / jnp.sum(l_ref[...], axis=1, keepdims=True)).astype(jnp.bfloat16)


ROUNDS = 4
PART = 256 // ROUNDS


def relay_kernel(
    cache, queries, bias, out, attended, keys, ybuf, z0, zbuf, kbuf, vbuf, qbuf, obuf, s_ref, m_ref, l_ref, acc_ref,
    y0s, y0r, y0o, ys, yr, yo, z0s, z0r, zs, zr, gs, gr, go, fs, fr, es, er, hs, hr, xs, xr, xo, oo, ks, vs, qs, os,
):
    d = lax.axis_index("doc")
    c = lax.axis_index("ctx")
    zl, y = d // 4, lax.rem(d, 4)
    x, zh, core = c // 4, lax.rem(c // 2, 2), lax.rem(c, 2)
    z = zh * 2 + zl
    chunk = zh * 2 + core
    sibling = place(x, y, z, 1 - core)
    partner = place(x, y, lax.rem(z + 2, 4), core)
    others = (1, 3, 2)

    def remote(src, dst, ssem, rsem, dev):
        return pltpu.make_async_remote_copy(src, dst, ssem, rsem, device_id=dev, device_id_type=MESH)

    def when_is(value, options, body):
        for v in options:
            @pl.when(value == v)
            def _():
                body(v)

    def slots(half, u):
        return pl.ds(pl.multiple_of(half * 256 + u * PART, PART), PART)

    def y0_copy(u, step):
        to = lax.rem(y + step, 4)
        rows = pl.ds(pl.multiple_of(u * PART, PART), PART)
        src = cache.at[0, :, to // 2, lax.rem(to, 2), :, rows]
        dst = ybuf.at[0, y // 2, lax.rem(y, 2), :, :, rows]
        if step == 0:
            return pltpu.make_async_copy(src, dst, y0o.at[u])
        return remote(src, dst, y0s.at[u, step - 1], y0r.at[u, step - 1], place(x, to, z, core))

    def y_copy(layer, step):
        to = lax.rem(y + step, 4)
        src = cache.at[layer, :, to // 2, lax.rem(to, 2)]
        dst = ybuf.at[layer, y // 2, lax.rem(y, 2)]
        if step == 0:
            return pltpu.make_async_copy(src, dst, yo.at[layer - 1])
        return remote(src, dst, ys.at[layer - 1, step - 1], yr.at[layer - 1, step - 1], place(x, to, z, core))

    def z0_copy(u, step, flip, both):
        to_z, to_core = lax.rem(z + step, 4), lax.rem(core + flip, 2)
        rows = pl.ds(pl.multiple_of(u * PART, PART), PART)
        r = step * 2 + flip
        if both:
            src = ybuf.at[0, :, :, lax.rem(to_z, 2), to_core, rows]
            dst = z0.at[chunk, pl.ds(zl * 2, 2), :, rows]
        else:
            src = ybuf.at[0, :, to_z // 2, lax.rem(to_z, 2), to_core, rows]
            dst = z0.at[chunk, pl.ds(zl * 2, 2), to_z // 2, rows]
        if r == 0:
            return pltpu.make_async_copy(src, dst, z0r.at[u, 0])
        return remote(src, dst, z0s.at[u, r], z0r.at[u, r], place(x, y, to_z, to_core))

    zorder = ((1, 0), (1, 1), (3, 0), (3, 1), (2, 0), (2, 1), (0, 1), (0, 0))

    def z0_send(u):
        for step in (1, 2, 3):
            y0_copy(u, step).wait_recv()
        y0_copy(u, 0).wait()

        def go_on(v):
            for step, flip in zorder:
                z0_copy(u, step, flip, v == 1).start()

        when_is(core, (0, 1), go_on)

    def z0_wait(u):
        def take(v):
            for step, flip in zorder:
                copy = z0_copy(u, step, flip, (v + flip) % 2 == 1)
                if step * 2 + flip == 0:
                    copy.wait()
                else:
                    copy.wait_recv()

        when_is(core, (0, 1), take)

    def span(ref, lead, piece, n, par, rows):
        if piece % 2:
            return ref.at[lead, pl.ds(0, n), :, rows]
        return ref.at[lead, pl.ds(0, n), par, rows]

    def near(piece, n, u):
        return span(z0, piece, piece, n, zh, pl.ds(pl.multiple_of(u * PART, PART), PART))

    def far(frm, piece, n, u):
        return span(keys, frm * 4 + piece, piece, n, zh, slots(core, u))

    def g_copy(u, piece, step, n):
        to = lax.rem(x + step, 4)
        return remote(near(piece, n, u), far(x, piece, n, u), gs.at[u, piece, step - 1], gr.at[u, piece, step - 1], place(to, y, z, core))

    def g_own(u, piece, n):
        return pltpu.make_async_copy(near(piece, n, u), far(x, piece, n, u), go.at[u, piece])

    def source(step):
        return lax.rem(x - step + 4, 4)

    def f_copy(u, piece, step, n):
        frm = source(step)
        dst = far(frm, piece, n, u)
        src = near(piece, n, u) if step == 0 else dst
        return remote(src, dst, fs.at[u, piece, step], fr.at[u, piece, step], sibling)

    def e_copy(u, piece, step, n):
        frm = source(step)
        dst = far(frm, piece, n, u)
        src = near(piece, n, u) if step == 0 else dst
        return remote(src, dst, es.at[u, piece // 2, step], er.at[u, piece // 2, step], partner)

    def h_copy(u, piece, step, n):
        here = keys.at[source(step) * 4 + piece, pl.ds(0, n), 1 - zh, slots(core, u)]
        return remote(here, here, hs.at[u, piece // 2, step], hr.at[u, piece // 2, step], sibling)

    given, taken = x + 1 - zh, x + zh

    def g_send(u):
        for step in others:
            def send(v):
                for piece in range(4):
                    g_copy(u, piece, step, v + 1).start()

            when_is(lax.rem(x + step, 4), range(4), send)

        def keep(v):
            for piece in range(4):
                f_copy(u, piece, 0, v + 1).start()
                g_own(u, piece, v + 1).start()

        when_is(x, range(4), keep)

        def swap(n):
            for piece in (0, 2):
                e_copy(u, piece, 0, n).start()

        when_is(given, range(1, 5), swap)

    def g_pass(u):
        for step in others:
            for piece in range(4):
                def take(v):
                    g_copy(u, piece, step, v + 1).wait_recv()
                    f_copy(u, piece, step, v + 1).start()

                when_is(x, range(4), take)
                if piece % 2 == 0:
                    when_is(given, range(1, 5), lambda n: e_copy(u, piece, step, n).start())

    def e_pass(u):
        def take(n):
            for step in (0,) + others:
                for piece in (0, 2):
                    e_copy(u, piece, step, n).wait_recv()
                    h_copy(u, piece, step, n).start()

        when_is(taken, range(1, 5), take)

    def own_row(piece, step):
        frm = source(step)
        cols = pl.ds(pl.multiple_of((frm * 4 + piece) * HD, HD), HD)
        if step == 0:
            src = z0.at[piece, x, zh]
        else:
            src = keys.at[frm * 4 + piece, x, zh, pl.ds(pl.multiple_of(core * 256, 256), 256)]
        return pltpu.make_async_copy(src, out.at[0, :, cols], oo.at[piece, step])

    def z_copy(layer, step, flip):
        to_z, to_core = lax.rem(z + step, 4), lax.rem(core + flip, 2)
        r = step * 2 + flip
        src = ybuf.at[layer, :, to_z // 2, lax.rem(to_z, 2), to_core]
        dst = zbuf.at[layer - 1, pl.ds(zl * 2, 2), chunk]
        if r == 0:
            return pltpu.make_async_copy(src, dst, zr.at[layer - 1, 0])
        return remote(src, dst, zs.at[layer - 1, r], zr.at[layer - 1, r], place(x, y, to_z, to_core))

    def x_copy(layer, step, piece):
        to = lax.rem(x + step, 4)
        cols = pl.ds(pl.multiple_of((x * 4 + piece) * HD, HD), HD)
        src = zbuf.at[layer - 1, to, piece]
        dst = out.at[layer, :, cols]
        if step == 0:
            return pltpu.make_async_copy(src, dst, xo.at[layer - 1, piece])
        return remote(src, dst, xs.at[layer - 1, step - 1, piece], xr.at[layer - 1, step - 1, piece], place(to, y, z, core))

    def z_send(layer):
        for step in (1, 2, 3):
            y_copy(layer, step).wait_recv()
        y_copy(layer, 0).wait()
        for step, flip in zorder:
            z_copy(layer, step, flip).start()

    def x_send(layer):
        for step, flip in zorder:
            if step * 2 + flip == 0:
                z_copy(layer, 0, 0).wait()
            else:
                z_copy(layer, step, flip).wait_recv()
        for step in (1, 3, 2, 0):
            for piece in range(4):
                x_copy(layer, step, piece).start()

    def q_copy(k, g):
        slot = lax.rem(k, 2)
        cols = pl.ds(pl.multiple_of((k * GROUP + g) * HD, HD), HD)
        return pltpu.make_async_copy(queries.at[:, cols], qbuf.at[slot, pl.ds(g * 256, 256)], qs.at[slot, g])

    def o_copy(k, g):
        slot = lax.rem(k, 2)
        cols = pl.ds(pl.multiple_of((k * GROUP + g) * HD, HD), HD)
        return pltpu.make_async_copy(obuf.at[slot, pl.ds(g * 256, 256)], attended.at[:, cols], os.at[slot, g])

    def kv_copies(k, n):
        slot = lax.rem(k, 2)
        return (
            pltpu.make_async_copy(keys.at[k, pl.ds(0, n)], kbuf.at[slot, pl.ds(0, n)], ks.at[slot]),
            pltpu.make_async_copy(keys.at[k + KVH, pl.ds(0, n)], vbuf.at[slot, pl.ds(0, n)], vs.at[slot]),
        )

    def fetch(k):
        for g in range(GROUP):
            q_copy(k, g).start()

        def body(v):
            for copy in kv_copies(k, v + 1):
                copy.start()

        when_is(x, range(4), body)

    def fetched(k):
        for g in range(GROUP):
            q_copy(k, g).wait()

        def body(v):
            for copy in kv_copies(k, v + 1):
                copy.wait()

        when_is(x, range(4), body)

    @pl.loop(0, ROUNDS)
    def _(u):
        for step in others + (0,):
            y0_copy(u, step).start()

    @pl.loop(1, LAYERS)
    def _(layer):
        for step in others + (0,):
            y_copy(layer, step).start()

    @pl.loop(0, ROUNDS + 2)
    def _(t):
        @pl.when(t < ROUNDS)
        def _():
            z0_send(t)

        @pl.when(t >= 2)
        def _():
            z0_wait(t - 2)
            g_send(t - 2)

    for piece in range(4):
        own_row(piece, 0).start()

    @pl.loop(1, LAYERS)
    def _(layer):
        z_send(layer)

        @pl.when(layer >= 2)
        def _():
            x_send(layer - 1)

        @pl.when((layer >= 2) & (layer < 2 + ROUNDS))
        def _():
            g_pass(layer - 2)

        @pl.when((layer >= 3) & (layer < 3 + ROUNDS))
        def _():
            e_pass(layer - 3)

    for piece in range(4):
        for step in others:
            own_row(piece, step).start()

    def settle(v):
        @pl.loop(0, ROUNDS)
        def _(u):
            for piece in range(4):
                g_own(u, piece, v + 1).wait()
                for step in range(4):
                    f_copy(u, piece, step, v + 1).wait()

    when_is(x, range(4), settle)

    def settle_h(n):
        @pl.loop(0, ROUNDS)
        def _(u):
            for piece in (0, 2):
                for step in range(4):
                    h_copy(u, piece, step, n).wait()

    when_is(taken, range(1, 5), settle_h)

    fetch(0)
    mine = x * 2 + zh

    @pl.loop(0, KVH)
    def _(k):
        fetched(k)

        @pl.when(k + 1 < KVH)
        def _():
            fetch(k + 1)

        @pl.when(k == 0)
        def _():
            x_send(LAYERS - 1)

        @pl.when(k >= 2)
        def _():
            for g in range(GROUP):
                o_copy(k - 2, g).wait()

        slot = lax.rem(k, 2)
        obuf[slot] = head_group(mine, core, qbuf.at[slot], kbuf.at[slot], vbuf.at[slot], bias, s_ref, m_ref, l_ref, acc_ref)
        for g in range(GROUP):
            o_copy(k, g).start()

    for k in (KVH - 2, KVH - 1):
        for g in range(GROUP):
            o_copy(k, g).wait()
    for piece in range(4):
        for step in range(4):
            own_row(piece, step).wait()

    @pl.loop(0, ROUNDS)
    def _(u):
        for step in others:
            y0_copy(u, step).wait_send()

            def sent(v):
                for piece in range(4):
                    g_copy(u, piece, step, v + 1).wait_send()

            when_is(lax.rem(x + step, 4), range(4), sent)

        def z_sent(v):
            for step, flip in zorder:
                if step * 2 + flip:
                    z0_copy(u, step, flip, v == 1).wait_send()

        when_is(core, (0, 1), z_sent)

        def swapped(n):
            for piece in (0, 2):
                for step in range(4):
                    e_copy(u, piece, step, n).wait_send()

        when_is(given, range(1, 5), swapped)

    @pl.loop(1, LAYERS)
    def _(layer):
        for step in others:
            y_copy(layer, step).wait_send()
        for step, flip in zorder:
            if step * 2 + flip:
                z_copy(layer, step, flip).wait_send()
        for piece in range(4):
            for step in range(4):
                x_copy(layer, step, piece).wait()


def relay(cache, queries, bias):
    dma = pltpu.SemaphoreType.DMA
    bf = jnp.bfloat16
    f32 = jnp.float32
    rows = GROUP * 256
    anyspace = pl.BlockSpec(memory_space=pl.ANY)
    sems = [
        (4, 3), (4, 3), (4,), (7, 3), (7, 3), (7,), (4, 8), (4, 8), (7, 8), (7, 8), (4, 4, 3), (4, 4, 3), (4, 4),
        (4, 4, 4), (4, 4, 4), (4, 2, 4), (4, 2, 4), (4, 2, 4), (4, 2, 4), (7, 3, 4), (7, 3, 4), (7, 4), (4, 4),
        (2,), (2,), (2, 4), (2, 4),
    ]
    return pl.pallas_call(
        relay_kernel,
        out_shape=(
            jax.ShapeDtypeStruct((LAYERS, 256, 2048), bf),
            jax.ShapeDtypeStruct((256, QH * HD), bf),
            jax.ShapeDtypeStruct((CHUNKS, 4, 2, SEQD, HD), bf),
            jax.ShapeDtypeStruct((LAYERS, 2, 2, 2, 2, 256, HD), bf),
        ),
        in_specs=[anyspace, anyspace, pl.BlockSpec(memory_space=pltpu.VMEM)],
        out_specs=(anyspace,) * 4,
        scratch_shapes=[
            pltpu.VMEM((4, 4, 2, 256, HD), bf),
            pltpu.VMEM((LAYERS - 1, 4, 4, 256, HD), bf),
            pltpu.VMEM((2, 4, 2, SEQD, HD), bf),
            pltpu.VMEM((2, 4, 2, SEQD, HD), bf),
            pltpu.VMEM((2, rows, HD), bf),
            pltpu.VMEM((2, rows, HD), bf),
            pltpu.VMEM((8, rows, SEQD), f32),
            pltpu.VMEM((rows, 128), f32),
            pltpu.VMEM((rows, 128), f32),
            pltpu.VMEM((rows, HD), f32),
        ]
        + [dma(shape) for shape in sems],
        compiler_params=pltpu.CompilerParams(has_side_effects=True, vmem_limit_bytes=56 << 20),
    )(cache.reshape(LAYERS, 2, 2, 2, 2, 256, HD), queries, bias)


def key_bias(section_counts, summary_blocks):
    chosen = (jnp.arange(8) == lax.axis_index("doc")).astype(jnp.int32)
    counts = jnp.sum(section_counts.reshape(8, 8) * chosen[None, :], axis=1)
    blocks = jnp.sum(summary_blocks.reshape(8, 8, SECTIONS) * chosen[None, :, None], axis=1)
    live_section = jnp.arange(SECTIONS)[None, :] < counts[:, None]
    live_slot = jnp.arange(SUMLEN)[None, None, :] < BLOCK * blocks[:, :, None]
    live = (live_section[:, :, None] & live_slot).reshape(8, SEQD)
    return jnp.where(live, 0.0, NEGATIVE).astype(jnp.float32)


def local(summary_cache, queries, section_counts, summary_blocks):
    bias = key_bias(section_counts, summary_blocks)
    relayed, attended, _, _ = relay(summary_cache, queries[0], bias)
    return attended[None], relayed[:, None]


def solution(mesh):
    placed = (P(None, "doc", None, "ctx"), P("doc", "ctx", None), P(), P())
    return jax.shard_map(
        local,
        mesh=mesh,
        in_specs=placed,
        out_specs=(P("doc", "ctx", None), P(None, "doc", "ctx", None)),
        check_vma=False,
    )
```

```python
import functools
import math

import jax
import jax.numpy as jnp
from jax import lax
from jax.experimental import pallas as pl
from jax.experimental.pallas import tpu as pltpu
from jax.sharding import PartitionSpec as P

QH = 32
KVH = 8
HD = 128
BLOCK = 128
SECTIONS = 2
GROUP = 4
SUMLEN = 256
SEQD = 512
LAYERS = 8
GSEQ = 4096
CHUNKS = 16
NEGATIVE = -1e30
MESH = pl.DeviceIdType.MESH
SCALE = (1.0 / math.sqrt(HD)) * math.log2(math.e)


def place(x, y, z, core):
    return (lax.rem(z, 2) * 4 + y, x * 4 + (z // 2) * 2 + core)


def head_group(mine, half, q_ref, k_ref, v_ref, bias_ref, s_ref, m_ref, l_ref, acc_ref):
    rows = q_ref.shape[0]

    def score(doc, diagonal):
        k = k_ref[doc // 2, lax.rem(doc, 2)]
        s = lax.dot_general(q_ref[...], k, (((1,), (1,)), ((), ())), preferred_element_type=jnp.float32)
        s = s * SCALE + bias_ref[pl.ds(doc, 1), :]
        if diagonal:
            at = lax.rem(lax.broadcasted_iota(jnp.int32, s.shape, 0), 256) + half * 256
            s = jnp.where(lax.broadcasted_iota(jnp.int32, s.shape, 1) <= at, s, NEGATIVE)
        s_ref[doc] = s
        top = jnp.maximum(jnp.maximum(s[:, 0:128], s[:, 128:256]), jnp.maximum(s[:, 256:384], s[:, 384:512]))
        return top

    def weigh(doc):
        v = v_ref[doc // 2, lax.rem(doc, 2)]
        top = m_ref[...]
        w = [jnp.exp2(s_ref[doc, :, i * 128 : (i + 1) * 128] - top) for i in range(4)]
        part = (w[0] + w[1]) + (w[2] + w[3])
        pair = [jnp.concatenate([w[2 * i].astype(jnp.bfloat16), w[2 * i + 1].astype(jnp.bfloat16)], axis=1) for i in range(2)]
        summed = lax.dot_general(
            jnp.concatenate(pair, axis=1), v, (((1,), (0,)), ((), ())), preferred_element_type=jnp.float32
        )
        return part, summed

    m_ref[...] = score(mine, True)

    @pl.loop(0, mine)
    def _(doc):
        m_ref[...] = jnp.maximum(m_ref[...], score(doc, False))

    m_ref[...] = jnp.broadcast_to(jnp.max(m_ref[...], axis=1, keepdims=True), m_ref.shape)
    part, summed = weigh(mine)
    l_ref[...] = part
    acc_ref[...] = summed

    @pl.loop(0, mine)
    def _(doc):
        part, summed = weigh(doc)
        l_ref[...] += part
        acc_ref[...] += summed

    return (acc_ref[...] / jnp.sum(l_ref[...], axis=1, keepdims=True)).astype(jnp.bfloat16)


ROUNDS = 4
PART = SEQD // ROUNDS


def relay_kernel(
    cache, queries, bias, out, attended, ybuf, keys, zbuf, qbuf, obuf, s_ref, m_ref, l_ref, acc_ref,
    y0s, y0r, y0o, ys, yr, yo, z0s, z0r, z0o, zs, zr, gs, gr, xs, xr, xo, ls, lr, qs, qr, os, rs,
):
    d = lax.axis_index("doc")
    c = lax.axis_index("ctx")
    zl, y = d // 4, lax.rem(d, 4)
    x, zh, core = c // 4, lax.rem(c // 2, 2), lax.rem(c, 2)
    z = zh * 2 + zl
    chunk = zh * 2 + core
    others = (1, 3, 2)

    def remote(src, dst, ssem, rsem, dev):
        return pltpu.make_async_remote_copy(src, dst, ssem, rsem, device_id=dev, device_id_type=MESH)

    def when_is(value, options, body):
        for v in options:
            @pl.when(value == v)
            def _():
                body(v)

    def part(u):
        return pl.ds(pl.multiple_of(u * PART, PART), PART)

    def half_rows(half):
        return pl.ds(pl.multiple_of(half * 256, 256), 256)

    def head_cols(h):
        return pl.ds(pl.multiple_of(h * HD, HD), HD)

    def y_copy(layer, step, u=None):
        to = lax.rem(y + step, 4)
        src = cache.at[layer, :, to // 2, lax.rem(to, 2)]
        dst = ybuf.at[layer, y // 2, lax.rem(y, 2)]
        if u is None:
            ssem, rsem, own, at = ys, yr, yo, layer - 1
        else:
            ssem, rsem, own, at = y0s, y0r, y0o, u
            src, dst = src.at[:, part(u)], dst.at[:, part(u)]
        if step == 0:
            return pltpu.make_async_copy(src, dst, own.at[at])
        return remote(src, dst, ssem.at[at, step - 1], rsem.at[at, step - 1], place(x, to, z, core))

    def y_wait(layer, u=None):
        for step in others:
            y_copy(layer, step, u).wait_recv()
        y_copy(layer, 0, u).wait()

    def z0_copy(u, flip):
        to = lax.rem(zl + flip, 2)
        src = ybuf.at[0, :, :, to, part(u)]
        dst = keys.at[x, pl.ds(zl * 2, 2), :, part(u)]
        if flip == 0:
            return pltpu.make_async_copy(src, dst, z0o.at[u])
        return remote(src, dst, z0s.at[u], z0r.at[u], place(x, y, zh * 2 + to, core))

    def g_copy(u, step, n):
        to = lax.rem(x + step, 4)
        ref = keys.at[x, pl.ds(0, n), :, part(u)]
        return remote(ref, ref, gs.at[u, step - 1], gr.at[u, step - 1], place(to, y, z, core))

    def peer(rel):
        return lax.rem(zh + rel // 2, 2), lax.rem(core + lax.rem(rel, 2), 2)

    def peer_place(rel):
        to_zh, to_core = peer(rel)
        return place(x, y, to_zh * 2 + zl, to_core)

    def l_copy(frm, rel):
        to_zh, to_core = peer(rel)
        src = keys.at[frm, x, to_zh, half_rows(to_core)]
        dst = out.at[0, :, head_cols(frm * 4 + chunk)]
        if rel == 0:
            return pltpu.make_async_copy(src, dst, lr.at[frm, 0])
        return remote(src, dst, ls.at[frm, rel], lr.at[frm, rel], peer_place(rel))

    def q_copy(kv, g, rel):
        to_zh, to_core = peer(rel)
        src = queries.at[:, head_cols((kv * 4 + to_zh * 2 + to_core) * GROUP + g)]
        dst = qbuf.at[kv, chunk, pl.ds(g * 256, 256)]
        if rel == 0:
            return pltpu.make_async_copy(src, dst, qr.at[kv, g, 0])
        return remote(src, dst, qs.at[kv, g, rel], qr.at[kv, g, rel], peer_place(rel))

    def o_copy(kv, g, rel, away):
        to_zh, to_core = peer(rel)
        src = obuf.at[kv, to_zh * 2 + to_core, pl.ds(g * 256, 256)]
        dst = attended.at[:, head_cols((kv * 4 + chunk) * GROUP + g)]
        if not away:
            return pltpu.make_async_copy(src, dst, rs.at[kv, g, 0])
        return remote(src, dst, os.at[kv, g, rel], rs.at[kv, g, rel], peer_place(rel))

    zorder = ((1, 0), (1, 1), (3, 0), (3, 1), (2, 0), (2, 1), (0, 1), (0, 0))

    def z_copy(layer, step, flip):
        to_z, to_core = lax.rem(z + step, 4), lax.rem(core + flip, 2)
        r = step * 2 + flip
        src = ybuf.at[layer, :, to_z // 2, lax.rem(to_z, 2), half_rows(to_core)]
        dst = zbuf.at[layer - 1, pl.ds(zl * 2, 2), chunk]
        if r == 0:
            return pltpu.make_async_copy(src, dst, zr.at[layer - 1, 0])
        return remote(src, dst, zs.at[layer - 1, r], zr.at[layer - 1, r], place(x, y, to_z, to_core))

    def x_copy(layer, step, piece):
        to = lax.rem(x + step, 4)
        src = zbuf.at[layer - 1, to, piece]
        dst = out.at[layer, :, head_cols(x * 4 + piece)]
        if step == 0:
            return pltpu.make_async_copy(src, dst, xo.at[layer - 1, piece])
        return remote(src, dst, xs.at[layer - 1, step - 1, piece], xr.at[layer - 1, step - 1, piece], place(to, y, z, core))

    def z_send(layer):
        y_wait(layer)
        for step, flip in zorder:
            z_copy(layer, step, flip).start()

    def x_send(layer):
        for step, flip in zorder:
            if step * 2 + flip == 0:
                z_copy(layer, 0, 0).wait()
            else:
                z_copy(layer, step, flip).wait_recv()
        for step in (1, 3, 2, 0):
            for piece in range(4):
                x_copy(layer, step, piece).start()

    @pl.loop(0, ROUNDS)
    def _(u):
        for step in others + (0,):
            y_copy(0, step, u).start()

    @pl.loop(1, LAYERS)
    def _(layer):
        for step in others + (0,):
            y_copy(layer, step).start()

    @pl.loop(0, ROUNDS + 1)
    def _(t):
        @pl.when(t < ROUNDS)
        def _():
            y_wait(0, t)
            z0_copy(t, 1).start()
            z0_copy(t, 0).start()

        @pl.when(t >= 1)
        def _():
            z0_copy(t - 1, 1).wait_recv()
            z0_copy(t - 1, 0).wait()
            for step in others:
                when_is(lax.rem(x + step, 4), range(4), lambda v: g_copy(t - 1, step, v + 1).start())

    for rel in (3, 2, 1, 0):
        for kv in range(2):
            for g in range(GROUP):
                q_copy(kv, g, rel).start()

    @pl.loop(1, 4)
    def _(layer):
        z_send(layer)

    def gathered(v):
        @pl.loop(0, ROUNDS)
        def _(u):
            for step in others:
                g_copy(u, step, v + 1).wait_recv()

    when_is(x, range(4), gathered)
    x_send(1)

    @pl.loop(0, 8)
    def _(t):
        rel = 3 - t // 2
        kv = lax.rem(t, 2)
        to_zh, to_core = peer(rel)
        for g in range(GROUP):
            pltpu.make_async_copy(queries.at[:, head_cols(g)], qbuf.at[kv, 0, pl.ds(g * 256, 256)], qr.at[kv, g, rel]).wait()
        src = to_zh * 2 + to_core
        obuf[kv, src] = head_group(
            x * 2 + to_zh, to_core, qbuf.at[kv, src], keys.at[kv], keys.at[2 + kv], bias, s_ref, m_ref, l_ref, acc_ref
        )

        @pl.when(t < 4)
        def _():
            z_send(t + 4)

        @pl.when(t < 6)
        def _():
            x_send(t + 2)
            for g in range(GROUP):
                o_copy(kv, g, rel, True).start()

        @pl.when(t >= 6)
        def _():
            for g in range(GROUP):
                o_copy(kv, g, 0, False).start()

        @pl.when(t == 4)
        def _():
            for rel in (3, 2, 1, 0):
                for frm in range(4):
                    l_copy(frm, rel).start()

    @pl.loop(0, ROUNDS)
    def _(u):
        for step in others:
            y_copy(0, step, u).wait_send()
            when_is(lax.rem(x + step, 4), range(4), lambda v: g_copy(u, step, v + 1).wait_send())
        z0_copy(u, 1).wait_send()

    for kv in range(2):
        for g in range(GROUP):
            o_copy(kv, g, 0, False).wait()
            for rel in (1, 2, 3):
                q_copy(kv, g, rel).wait_send()
                o_copy(kv, g, rel, True).wait()

    for frm in range(4):
        for rel in range(4):
            l_copy(frm, rel).wait()

    @pl.loop(1, LAYERS)
    def _(layer):
        for step in others:
            y_copy(layer, step).wait_send()
        for step, flip in zorder:
            if step * 2 + flip:
                z_copy(layer, step, flip).wait_send()
        for piece in range(4):
            for step in range(4):
                x_copy(layer, step, piece).wait()


def relay(cache, queries, bias):
    dma = pltpu.SemaphoreType.DMA
    bf = jnp.bfloat16
    f32 = jnp.float32
    rows = GROUP * 256
    anyspace = pl.BlockSpec(memory_space=pl.ANY)
    sems = [
        (4, 3), (4, 3), (4,), (7, 3), (7, 3), (7,), (4,), (4,), (4,), (7, 8), (7, 8), (4, 3), (4, 3),
        (7, 3, 4), (7, 3, 4), (7, 4), (4, 4), (4, 4), (2, 4, 4), (2, 4, 4), (2, 4, 4), (2, 4, 4),
    ]
    return pl.pallas_call(
        relay_kernel,
        out_shape=(
            jax.ShapeDtypeStruct((LAYERS, 256, 2048), bf),
            jax.ShapeDtypeStruct((256, QH * HD), bf),
            jax.ShapeDtypeStruct((LAYERS, 2, 2, 2, SEQD, HD), bf),
        ),
        in_specs=[anyspace, anyspace, pl.BlockSpec(memory_space=pltpu.VMEM)],
        out_specs=(anyspace,) * 3,
        scratch_shapes=[
            pltpu.VMEM((4, 4, 2, SEQD, HD), bf),
            pltpu.VMEM((LAYERS - 1, 4, 4, 256, HD), bf),
            pltpu.VMEM((2, 4, rows, HD), bf),
            pltpu.VMEM((2, 4, rows, HD), bf),
            pltpu.VMEM((8, rows, SEQD), f32),
            pltpu.VMEM((rows, 128), f32),
            pltpu.VMEM((rows, 128), f32),
            pltpu.VMEM((rows, HD), f32),
        ]
        + [dma(shape) for shape in sems],
        compiler_params=pltpu.CompilerParams(has_side_effects=True, vmem_limit_bytes=56 << 20),
    )(cache.reshape(LAYERS, 2, 2, 2, SEQD, HD), queries, bias)


def key_bias(section_counts, summary_blocks):
    chosen = (jnp.arange(8) == lax.axis_index("doc")).astype(jnp.int32)
    counts = jnp.sum(section_counts.reshape(8, 8) * chosen[None, :], axis=1)
    blocks = jnp.sum(summary_blocks.reshape(8, 8, SECTIONS) * chosen[None, :, None], axis=1)
    live_section = jnp.arange(SECTIONS)[None, :] < counts[:, None]
    live_slot = jnp.arange(SUMLEN)[None, None, :] < BLOCK * blocks[:, :, None]
    live = (live_section[:, :, None] & live_slot).reshape(8, SEQD)
    return jnp.where(live, 0.0, NEGATIVE).astype(jnp.float32)


def local(summary_cache, queries, section_counts, summary_blocks):
    bias = key_bias(section_counts, summary_blocks)
    relayed, attended, _ = relay(summary_cache, queries[0], bias)
    return attended[None], relayed[:, None]


def solution(mesh):
    placed = (P(None, "doc", None, "ctx"), P("doc", "ctx", None), P(), P())
    return jax.shard_map(
        local,
        mesh=mesh,
        in_specs=placed,
        out_specs=(P("doc", "ctx", None), P(None, "doc", "ctx", None)),
        check_vma=False,
    )
```

```python
import functools
import math

import jax
import jax.numpy as jnp
from jax import lax
from jax.experimental import pallas as pl
from jax.experimental.pallas import tpu as pltpu
from jax.sharding import PartitionSpec as P

QH = 32
KVH = 8
HD = 128
BLOCK = 128
SECTIONS = 2
GROUP = 4
SUMLEN = 256
SEQD = 512
LAYERS = 8
GSEQ = 4096
CHUNKS = 16
NEGATIVE = -1e30
MESH = pl.DeviceIdType.MESH
SCALE = (1.0 / math.sqrt(HD)) * math.log2(math.e)


def place(x, y, z, core):
    return (lax.rem(z, 2) * 4 + y, x * 4 + (z // 2) * 2 + core)


def head_group(mine, half, q_ref, k_ref, v_ref, bias_ref, s_ref, m_ref, l_ref, acc_ref):
    rows = q_ref.shape[0]

    def score(doc, diagonal):
        k = k_ref[doc // 2, lax.rem(doc, 2)]
        s = lax.dot_general(q_ref[...], k, (((1,), (1,)), ((), ())), preferred_element_type=jnp.float32)
        s = s * SCALE + bias_ref[pl.ds(doc, 1), :]
        if diagonal:
            at = lax.rem(lax.broadcasted_iota(jnp.int32, s.shape, 0), 256) + half * 256
            s = jnp.where(lax.broadcasted_iota(jnp.int32, s.shape, 1) <= at, s, NEGATIVE)
        s_ref[doc] = s
        top = jnp.maximum(jnp.maximum(s[:, 0:128], s[:, 128:256]), jnp.maximum(s[:, 256:384], s[:, 384:512]))
        return top

    def weigh(doc):
        v = v_ref[doc // 2, lax.rem(doc, 2)]
        top = m_ref[...]
        w = [jnp.exp2(s_ref[doc, :, i * 128 : (i + 1) * 128] - top) for i in range(4)]
        part = (w[0] + w[1]) + (w[2] + w[3])
        pair = [jnp.concatenate([w[2 * i].astype(jnp.bfloat16), w[2 * i + 1].astype(jnp.bfloat16)], axis=1) for i in range(2)]
        summed = lax.dot_general(
            jnp.concatenate(pair, axis=1), v, (((1,), (0,)), ((), ())), preferred_element_type=jnp.float32
        )
        return part, summed

    m_ref[...] = score(mine, True)

    @pl.loop(0, mine)
    def _(doc):
        m_ref[...] = jnp.maximum(m_ref[...], score(doc, False))

    m_ref[...] = jnp.broadcast_to(jnp.max(m_ref[...], axis=1, keepdims=True), m_ref.shape)
    part, summed = weigh(mine)
    l_ref[...] = part
    acc_ref[...] = summed

    @pl.loop(0, mine)
    def _(doc):
        part, summed = weigh(doc)
        l_ref[...] += part
        acc_ref[...] += summed

    return (acc_ref[...] / jnp.sum(l_ref[...], axis=1, keepdims=True)).astype(jnp.bfloat16)


ROUNDS = 4
PART = SEQD // ROUNDS


def relay_kernel(
    cache, queries, bias, out, attended, ybuf, keys, zbuf, qbuf, obuf, s_ref, m_ref, l_ref, acc_ref,
    y0s, y0r, y0o, ys, yr, yo, z0s, z0r, z0o, zs, zr, gs, gr, xs, xr, ls, lr, qs, qr, os, rs,
):
    d = lax.axis_index("doc")
    c = lax.axis_index("ctx")
    zl, y = d // 4, lax.rem(d, 4)
    x, zh, core = c // 4, lax.rem(c // 2, 2), lax.rem(c, 2)
    z = zh * 2 + zl
    chunk = zh * 2 + core
    others = (1, 3, 2)

    def remote(src, dst, ssem, rsem, dev):
        return pltpu.make_async_remote_copy(src, dst, ssem, rsem, device_id=dev, device_id_type=MESH)

    def when_is(value, options, body):
        for v in options:
            @pl.when(value == v)
            def _():
                body(v)

    def part(u):
        return pl.ds(pl.multiple_of(u * PART, PART), PART)

    def half_rows(half):
        return pl.ds(pl.multiple_of(half * 256, 256), 256)

    def head_cols(h):
        return pl.ds(pl.multiple_of(h * HD, HD), HD)

    def y_copy(layer, step, u=None):
        to = lax.rem(y + step, 4)
        src = cache.at[layer, :, to // 2, lax.rem(to, 2)]
        dst = ybuf.at[layer, y // 2, lax.rem(y, 2)]
        if u is None:
            ssem, rsem, own, at = ys, yr, yo, layer - 1
        else:
            ssem, rsem, own, at = y0s, y0r, y0o, u
            src, dst = src.at[:, part(u)], dst.at[:, part(u)]
        if step == 0:
            return pltpu.make_async_copy(src, dst, own.at[at])
        return remote(src, dst, ssem.at[at, step - 1], rsem.at[at, step - 1], place(x, to, z, core))

    def y_wait(layer, u=None):
        for step in others:
            y_copy(layer, step, u).wait_recv()
        y_copy(layer, 0, u).wait()

    def z0_copy(u, flip):
        to = lax.rem(zl + flip, 2)
        src = ybuf.at[0, :, :, to, part(u)]
        dst = keys.at[x, pl.ds(zl * 2, 2), :, part(u)]
        if flip == 0:
            return pltpu.make_async_copy(src, dst, z0o.at[u])
        return remote(src, dst, z0s.at[u], z0r.at[u], place(x, y, zh * 2 + to, core))

    def g_copy(u, step, n):
        to = lax.rem(x + step, 4)
        ref = keys.at[x, pl.ds(0, n), :, part(u)]
        return remote(ref, ref, gs.at[u, step - 1], gr.at[u, step - 1], place(to, y, z, core))

    def peer(rel):
        return lax.rem(zh + rel // 2, 2), lax.rem(core + lax.rem(rel, 2), 2)

    def peer_place(rel):
        to_zh, to_core = peer(rel)
        return place(x, y, to_zh * 2 + zl, to_core)

    def l_copy(frm, rel):
        to_zh, to_core = peer(rel)
        src = keys.at[frm, x, to_zh, half_rows(to_core)]
        dst = out.at[0, :, head_cols(frm * 4 + chunk)]
        return remote(src, dst, ls.at[frm, rel], lr.at[frm, rel], peer_place(rel))

    def q_copy(kv, g, rel):
        to_zh, to_core = peer(rel)
        src = queries.at[:, head_cols((kv * 4 + to_zh * 2 + to_core) * GROUP + g)]
        dst = qbuf.at[kv, chunk, pl.ds(g * 256, 256)]
        if rel == 0:
            return pltpu.make_async_copy(src, dst, qr.at[kv, g, 0])
        return remote(src, dst, qs.at[kv, g, rel], qr.at[kv, g, rel], peer_place(rel))

    def o_copy(kv, g, rel):
        to_zh, to_core = peer(rel)
        src = obuf.at[kv, to_zh * 2 + to_core, pl.ds(g * 256, 256)]
        dst = attended.at[:, head_cols((kv * 4 + chunk) * GROUP + g)]
        return remote(src, dst, os.at[kv, g, rel], rs.at[kv, g, rel], peer_place(rel))

    zorder = ((1, 0), (1, 1), (3, 0), (3, 1), (2, 0), (2, 1), (0, 1), (0, 0))

    def z_copy(layer, step, flip):
        to_z, to_core = lax.rem(z + step, 4), lax.rem(core + flip, 2)
        r = step * 2 + flip
        src = ybuf.at[layer, :, to_z // 2, lax.rem(to_z, 2), half_rows(to_core)]
        dst = zbuf.at[layer - 1, pl.ds(zl * 2, 2), chunk]
        if r == 0:
            return pltpu.make_async_copy(src, dst, zr.at[layer - 1, 0])
        return remote(src, dst, zs.at[layer - 1, r], zr.at[layer - 1, r], place(x, y, to_z, to_core))

    def x_copy(layer, step, piece):
        to = lax.rem(x + step, 4)
        src = zbuf.at[layer - 1, to, piece]
        dst = out.at[layer, :, head_cols(x * 4 + piece)]
        return remote(src, dst, xs.at[layer - 1, step - 1, piece], xr.at[layer - 1, step - 1, piece], place(to, y, z, core))

    def z_send(layer):
        y_wait(layer)
        for step, flip in zorder:
            z_copy(layer, step, flip).start()

    def x_send(layer):
        for step, flip in zorder:
            if step * 2 + flip == 0:
                z_copy(layer, 0, 0).wait()
            else:
                z_copy(layer, step, flip).wait_recv()
        for step in others:
            for piece in range(4):
                x_copy(layer, step, piece).start()
        for piece in range(4):
            out[layer, :, head_cols(x * 4 + piece)] = zbuf[layer - 1, x, piece]

    @pl.loop(0, ROUNDS)
    def _(u):
        for step in others + (0,):
            y_copy(0, step, u).start()

    @pl.loop(1, LAYERS)
    def _(layer):
        for step in others + (0,):
            y_copy(layer, step).start()

    def q_send(kv, g):
        for rel in (3, 2, 1, 0):
            q_copy(kv, g, rel).start()

    for g in range(2):
        q_send(0, g)

    @pl.loop(0, ROUNDS + 1)
    def _(t):
        @pl.when(t < ROUNDS)
        def _():
            y_wait(0, t)
            z0_copy(t, 1).start()
            z0_copy(t, 0).start()

        @pl.when(t >= 1)
        def _():
            z0_copy(t - 1, 1).wait_recv()
            z0_copy(t - 1, 0).wait()
            for step in others:
                when_is(lax.rem(x + step, 4), range(4), lambda v: g_copy(t - 1, step, v + 1).start())

        when_is(t, range(2), lambda v: q_send(0, 2 + v))
        when_is(t, range(2, 4), lambda v: q_send(1, v - 2))

    for g in range(2, GROUP):
        q_send(1, g)

    @pl.loop(1, 4)
    def _(layer):
        z_send(layer)

    def gathered(v):
        @pl.loop(0, ROUNDS)
        def _(u):
            for step in others:
                g_copy(u, step, v + 1).wait_recv()

    when_is(x, range(4), gathered)
    x_send(1)

    @pl.loop(0, 8)
    def _(t):
        rel = 3 - t // 2
        kv = lax.rem(t, 2)
        to_zh, to_core = peer(rel)
        for g in range(GROUP):
            pltpu.make_async_copy(queries.at[:, head_cols(g)], qbuf.at[kv, 0, pl.ds(g * 256, 256)], qr.at[kv, g, rel]).wait()
        src = to_zh * 2 + to_core
        obuf[kv, src] = head_group(
            x * 2 + to_zh, to_core, qbuf.at[kv, src], keys.at[kv], keys.at[2 + kv], bias, s_ref, m_ref, l_ref, acc_ref
        )

        @pl.when(t < 4)
        def _():
            z_send(t + 4)

        @pl.when((t < 6) & (t != 2))
        def _():
            x_send(t + 2 - t // 3)

        @pl.when(t == 3)
        def _():
            for rel in (3, 2):
                for kv in range(2):
                    for g in range(GROUP):
                        o_copy(kv, g, rel).start()

        @pl.when((t == 4) | (t == 5))
        def _():
            for g in range(GROUP):
                o_copy(kv, g, 1).start()

        @pl.when(t >= 6)
        def _():
            for g in range(GROUP):
                attended[:, head_cols((kv * 4 + chunk) * GROUP + g)] = obuf[kv, chunk, pl.ds(g * 256, 256)]

        @pl.when(t == 4)
        def _():
            for rel in (3, 2, 1):
                for frm in range(4):
                    l_copy(frm, rel).start()
            for frm in range(4):
                out[0, :, head_cols(frm * 4 + chunk)] = keys[frm, x, zh, half_rows(core)]

        @pl.when(t == 7)
        def _():
            x_send(7)

    @pl.loop(0, ROUNDS)
    def _(u):
        for step in others:
            y_copy(0, step, u).wait_send()
            when_is(lax.rem(x + step, 4), range(4), lambda v: g_copy(u, step, v + 1).wait_send())
        z0_copy(u, 1).wait_send()

    for kv in range(2):
        for g in range(GROUP):
            for rel in (1, 2, 3):
                q_copy(kv, g, rel).wait_send()
                o_copy(kv, g, rel).wait()

    for frm in range(4):
        for rel in (1, 2, 3):
            l_copy(frm, rel).wait()

    @pl.loop(1, LAYERS)
    def _(layer):
        for step in others:
            y_copy(layer, step).wait_send()
        for step, flip in zorder:
            if step * 2 + flip:
                z_copy(layer, step, flip).wait_send()
        for piece in range(4):
            for step in others:
                x_copy(layer, step, piece).wait()


def relay(cache, queries, bias):
    dma = pltpu.SemaphoreType.DMA
    bf = jnp.bfloat16
    f32 = jnp.float32
    rows = GROUP * 256
    anyspace = pl.BlockSpec(memory_space=pl.ANY)
    sems = [
        (4, 3), (4, 3), (4,), (7, 3), (7, 3), (7,), (4,), (4,), (4,), (7, 8), (7, 8), (4, 3), (4, 3),
        (7, 3, 4), (7, 3, 4), (4, 4), (4, 4), (2, 4, 4), (2, 4, 4), (2, 4, 4), (2, 4, 4),
    ]
    return pl.pallas_call(
        relay_kernel,
        out_shape=(
            jax.ShapeDtypeStruct((LAYERS, 256, 2048), bf),
            jax.ShapeDtypeStruct((256, QH * HD), bf),
            jax.ShapeDtypeStruct((LAYERS, 2, 2, 2, SEQD, HD), bf),
        ),
        in_specs=[pl.BlockSpec(memory_space=pltpu.HBM)] * 2 + [pl.BlockSpec(memory_space=pltpu.VMEM)],
        out_specs=(pl.BlockSpec(memory_space=pltpu.VMEM),) * 2 + (anyspace,),
        scratch_shapes=[
            pltpu.VMEM((4, 4, 2, SEQD, HD), bf),
            pltpu.VMEM((LAYERS - 1, 4, 4, 256, HD), bf),
            pltpu.VMEM((2, 4, rows, HD), bf),
            pltpu.VMEM((2, 4, rows, HD), bf),
            pltpu.VMEM((8, rows, SEQD), f32),
            pltpu.VMEM((rows, 128), f32),
            pltpu.VMEM((rows, 128), f32),
            pltpu.VMEM((rows, HD), f32),
        ]
        + [dma(shape) for shape in sems],
        compiler_params=pltpu.CompilerParams(has_side_effects=True, vmem_limit_bytes=40 << 20),
    )(cache.reshape(LAYERS, 2, 2, 2, SEQD, HD), queries, bias)


def settle_kernel(out, attended, out_to, attended_to, sems):
    copies = [pltpu.make_async_copy(out.at[layer], out_to.at[layer], sems.at[layer]) for layer in range(LAYERS)]
    copies.append(pltpu.make_async_copy(attended, attended_to, sems.at[LAYERS]))
    for copy in copies:
        copy.start()
    for copy in copies:
        copy.wait()


def settle(out, attended):
    vmem, anyspace = pl.BlockSpec(memory_space=pltpu.VMEM), pl.BlockSpec(memory_space=pl.ANY)
    return pl.pallas_call(
        settle_kernel,
        out_shape=tuple(jax.ShapeDtypeStruct(a.shape, a.dtype) for a in (out, attended)),
        in_specs=[vmem, vmem],
        out_specs=(anyspace, anyspace),
        scratch_shapes=[pltpu.SemaphoreType.DMA((LAYERS + 1,))],
        compiler_params=pltpu.CompilerParams(vmem_limit_bytes=16 << 20),
    )(out, attended)


def key_bias(section_counts, summary_blocks):
    chosen = (jnp.arange(8) == lax.axis_index("doc")).astype(jnp.int32)
    counts = jnp.sum(section_counts.reshape(8, 8) * chosen[None, :], axis=1)
    blocks = jnp.sum(summary_blocks.reshape(8, 8, SECTIONS) * chosen[None, :, None], axis=1)
    live_section = jnp.arange(SECTIONS)[None, :] < counts[:, None]
    live_slot = jnp.arange(SUMLEN)[None, None, :] < BLOCK * blocks[:, :, None]
    live = (live_section[:, :, None] & live_slot).reshape(8, SEQD)
    return jnp.where(live, 0.0, NEGATIVE).astype(jnp.float32)


def local(summary_cache, queries, section_counts, summary_blocks):
    bias = key_bias(section_counts, summary_blocks)
    relayed, attended, _ = relay(summary_cache, queries[0], bias)
    relayed, attended = settle(relayed, attended)
    return attended[None], relayed[:, None]


def solution(mesh):
    placed = (P(None, "doc", None, "ctx"), P("doc", "ctx", None), P(), P())
    return jax.shard_map(
        local,
        mesh=mesh,
        in_specs=placed,
        out_specs=(P("doc", "ctx", None), P(None, "doc", "ctx", None)),
        check_vma=False,
    )
```

```python
import functools
import math

import jax
import jax.numpy as jnp
from jax import lax
from jax.experimental import pallas as pl
from jax.experimental.pallas import tpu as pltpu
from jax.sharding import PartitionSpec as P

QH = 32
KVH = 8
HD = 128
BLOCK = 128
SECTIONS = 2
GROUP = 4
SUMLEN = 256
SEQD = 512
LAYERS = 8
GSEQ = 4096
CHUNKS = 16
NEGATIVE = -1e30
MESH = pl.DeviceIdType.MESH
SCALE = (1.0 / math.sqrt(HD)) * math.log2(math.e)


def place(x, y, z, core):
    return (lax.rem(z, 2) * 4 + y, x * 4 + (z // 2) * 2 + core)


def head_group(mine, half, q_ref, k_ref, v_ref, bias_ref, s_ref, m_ref, l_ref, acc_ref):
    rows = q_ref.shape[0]

    def score(doc, diagonal):
        k = k_ref[doc // 2, lax.rem(doc, 2)]
        s = lax.dot_general(q_ref[...], k, (((1,), (1,)), ((), ())), preferred_element_type=jnp.float32)
        s = s * SCALE + bias_ref[pl.ds(doc, 1), :]
        if diagonal:
            at = lax.rem(lax.broadcasted_iota(jnp.int32, s.shape, 0), 256) + half * 256
            s = jnp.where(lax.broadcasted_iota(jnp.int32, s.shape, 1) <= at, s, NEGATIVE)
        s_ref[doc] = s
        top = jnp.maximum(jnp.maximum(s[:, 0:128], s[:, 128:256]), jnp.maximum(s[:, 256:384], s[:, 384:512]))
        return top

    def weigh(doc):
        v = v_ref[doc // 2, lax.rem(doc, 2)]
        top = m_ref[...]
        w = [jnp.exp2(s_ref[doc, :, i * 128 : (i + 1) * 128] - top) for i in range(4)]
        part = (w[0] + w[1]) + (w[2] + w[3])
        pair = [jnp.concatenate([w[2 * i].astype(jnp.bfloat16), w[2 * i + 1].astype(jnp.bfloat16)], axis=1) for i in range(2)]
        summed = lax.dot_general(
            jnp.concatenate(pair, axis=1), v, (((1,), (0,)), ((), ())), preferred_element_type=jnp.float32
        )
        return part, summed

    m_ref[...] = score(mine, True)

    @pl.loop(0, mine)
    def _(doc):
        m_ref[...] = jnp.maximum(m_ref[...], score(doc, False))

    m_ref[...] = jnp.broadcast_to(jnp.max(m_ref[...], axis=1, keepdims=True), m_ref.shape)
    part, summed = weigh(mine)
    l_ref[...] = part
    acc_ref[...] = summed

    @pl.loop(0, mine)
    def _(doc):
        part, summed = weigh(doc)
        l_ref[...] += part
        acc_ref[...] += summed

    return (acc_ref[...] / jnp.sum(l_ref[...], axis=1, keepdims=True)).astype(jnp.bfloat16)


ROUNDS = 4
PART = SEQD // ROUNDS


def relay_kernel(
    cache, queries, counts_hbm, blocks_hbm, out, attended, ybuf, bias, counts, blocks, keys, zbuf, qbuf, obuf, s_ref, m_ref, l_ref, acc_ref,
    y0s, y0r, y0o, ys, yr, yo, z0s, z0r, z0o, zs, zr, gs, gr, xs, xr, ls, lr, qs, qr, os, rs, cs,
):
    d = lax.axis_index("doc")
    c = lax.axis_index("ctx")
    zl, y = d // 4, lax.rem(d, 4)
    x, zh, core = c // 4, lax.rem(c // 2, 2), lax.rem(c, 2)
    z = zh * 2 + zl
    chunk = zh * 2 + core
    others = (1, 3, 2)

    def remote(src, dst, ssem, rsem, dev):
        return pltpu.make_async_remote_copy(src, dst, ssem, rsem, device_id=dev, device_id_type=MESH)

    def when_is(value, options, body):
        for v in options:
            @pl.when(value == v)
            def _():
                body(v)

    def part(u):
        return pl.ds(pl.multiple_of(u * PART, PART), PART)

    def half_rows(half):
        return pl.ds(pl.multiple_of(half * 256, 256), 256)

    def head_cols(h):
        return pl.ds(pl.multiple_of(h * HD, HD), HD)

    def y_copy(layer, step, u=None):
        to = lax.rem(y + step, 4)
        src = cache.at[layer, :, to // 2, lax.rem(to, 2)]
        dst = ybuf.at[layer, y // 2, lax.rem(y, 2)]
        if u is None:
            ssem, rsem, own, at = ys, yr, yo, layer - 1
        else:
            ssem, rsem, own, at = y0s, y0r, y0o, u
            src, dst = src.at[:, part(u)], dst.at[:, part(u)]
        if step == 0:
            return pltpu.make_async_copy(src, dst, own.at[at])
        return remote(src, dst, ssem.at[at, step - 1], rsem.at[at, step - 1], place(x, to, z, core))

    def y_wait(layer, u=None):
        for step in others:
            y_copy(layer, step, u).wait_recv()
        y_copy(layer, 0, u).wait()

    def z0_copy(u, flip):
        to = lax.rem(zl + flip, 2)
        src = ybuf.at[0, :, :, to, part(u)]
        dst = keys.at[x, pl.ds(zl * 2, 2), :, part(u)]
        if flip == 0:
            return pltpu.make_async_copy(src, dst, z0o.at[u])
        return remote(src, dst, z0s.at[u], z0r.at[u], place(x, y, zh * 2 + to, core))

    def g_copy(u, step, n):
        to = lax.rem(x + step, 4)
        ref = keys.at[x, pl.ds(0, n), :, part(u)]
        return remote(ref, ref, gs.at[u, step - 1], gr.at[u, step - 1], place(to, y, z, core))

    def peer(rel):
        return lax.rem(zh + rel // 2, 2), lax.rem(core + lax.rem(rel, 2), 2)

    def peer_place(rel):
        to_zh, to_core = peer(rel)
        return place(x, y, to_zh * 2 + zl, to_core)

    def l_copy(frm, rel):
        to_zh, to_core = peer(rel)
        src = keys.at[frm, x, to_zh, half_rows(to_core)]
        dst = out.at[0, :, head_cols(frm * 4 + chunk)]
        return remote(src, dst, ls.at[frm, rel], lr.at[frm, rel], peer_place(rel))

    def q_copy(kv, g, rel):
        to_zh, to_core = peer(rel)
        src = queries.at[:, head_cols((kv * 4 + to_zh * 2 + to_core) * GROUP + g)]
        dst = qbuf.at[kv, chunk, pl.ds(g * 256, 256)]
        if rel == 0:
            return pltpu.make_async_copy(src, dst, qr.at[kv, g, 0])
        return remote(src, dst, qs.at[kv, g, rel], qr.at[kv, g, rel], peer_place(rel))

    def o_copy(kv, g, rel):
        to_zh, to_core = peer(rel)
        src = obuf.at[kv, to_zh * 2 + to_core, pl.ds(g * 256, 256)]
        dst = attended.at[:, head_cols((kv * 4 + chunk) * GROUP + g)]
        return remote(src, dst, os.at[kv, g, rel], rs.at[kv, g, rel], peer_place(rel))

    zorder = ((1, 0), (1, 1), (3, 0), (3, 1), (2, 0), (2, 1), (0, 1), (0, 0))

    def z_copy(layer, step, flip):
        to_z, to_core = lax.rem(z + step, 4), lax.rem(core + flip, 2)
        r = step * 2 + flip
        src = ybuf.at[layer, :, to_z // 2, lax.rem(to_z, 2), half_rows(to_core)]
        dst = zbuf.at[layer - 1, pl.ds(zl * 2, 2), chunk]
        if r == 0:
            return pltpu.make_async_copy(src, dst, zr.at[layer - 1, 0])
        return remote(src, dst, zs.at[layer - 1, r], zr.at[layer - 1, r], place(x, y, to_z, to_core))

    def x_copy(layer, step, piece):
        to = lax.rem(x + step, 4)
        src = zbuf.at[layer - 1, to, piece]
        dst = out.at[layer, :, head_cols(x * 4 + piece)]
        return remote(src, dst, xs.at[layer - 1, step - 1, piece], xr.at[layer - 1, step - 1, piece], place(to, y, z, core))

    def z_send(layer):
        y_wait(layer)
        for step, flip in zorder:
            z_copy(layer, step, flip).start()

    def x_send(layer):
        for step, flip in zorder:
            if step * 2 + flip == 0:
                z_copy(layer, 0, 0).wait()
            else:
                z_copy(layer, step, flip).wait_recv()
        for step in others:
            for piece in range(4):
                x_copy(layer, step, piece).start()
        for piece in range(4):
            out[layer, :, head_cols(x * 4 + piece)] = zbuf[layer - 1, x, piece]

    barrier = pltpu.get_barrier_semaphore()
    peers = [place(x, lax.rem(y + step, 4), z, core) for step in others]
    peers += [place(lax.rem(x + step, 4), y, z, core) for step in others]
    peers += [place(x, y, lax.rem(z + step, 4), lax.rem(core + flip, 2)) for step, flip in zorder if step or flip]
    for peer_device in peers:
        pl.semaphore_signal(barrier, inc=1, device_id=peer_device, device_id_type=MESH)
    tables = [pltpu.make_async_copy(counts_hbm, counts, cs.at[0]), pltpu.make_async_copy(blocks_hbm, blocks, cs.at[1])]
    for copy in tables:
        copy.start()
    for u in range(ROUNDS):
        y_copy(0, 0, u).start()
    pl.semaphore_wait(barrier, len(peers))

    @pl.loop(0, ROUNDS)
    def _(u):
        for step in others:
            y_copy(0, step, u).start()

    @pl.loop(1, LAYERS)
    def _(layer):
        for step in others + (0,):
            y_copy(layer, step).start()

    def q_send(kv, g):
        for rel in (3, 2, 1, 0):
            q_copy(kv, g, rel).start()

    for g in range(2):
        q_send(0, g)

    @pl.loop(0, ROUNDS + 1)
    def _(t):
        @pl.when(t < ROUNDS)
        def _():
            y_wait(0, t)
            z0_copy(t, 1).start()
            z0_copy(t, 0).start()

        @pl.when(t >= 1)
        def _():
            z0_copy(t - 1, 1).wait_recv()
            z0_copy(t - 1, 0).wait()
            for step in others:
                when_is(lax.rem(x + step, 4), range(4), lambda v: g_copy(t - 1, step, v + 1).start())

        when_is(t, range(2), lambda v: q_send(0, 2 + v))
        when_is(t, range(2, 4), lambda v: q_send(1, v - 2))

    for g in range(2, GROUP):
        q_send(1, g)

    for copy in tables:
        copy.wait()
    slot = lax.broadcasted_iota(jnp.int32, (1, SEQD), 1)
    second = slot // SUMLEN
    for doc in range(8):
        at = doc * 8 + d
        live_blocks = jnp.where(second == 0, blocks[at, 0], blocks[at, 1])
        live = (second < counts[at]) & (slot - second * SUMLEN < BLOCK * live_blocks)
        bias[doc : doc + 1, :] = jnp.where(live, 0.0, NEGATIVE)

    @pl.loop(1, 4)
    def _(layer):
        z_send(layer)

    def gathered(v):
        @pl.loop(0, ROUNDS)
        def _(u):
            for step in others:
                g_copy(u, step, v + 1).wait_recv()

    when_is(x, range(4), gathered)
    x_send(1)

    @pl.loop(0, 8)
    def _(t):
        rel = 3 - t // 2
        kv = lax.rem(t, 2)
        to_zh, to_core = peer(rel)
        for g in range(GROUP):
            pltpu.make_async_copy(queries.at[:, head_cols(g)], qbuf.at[kv, 0, pl.ds(g * 256, 256)], qr.at[kv, g, rel]).wait()
        src = to_zh * 2 + to_core
        obuf[kv, src] = head_group(
            x * 2 + to_zh, to_core, qbuf.at[kv, src], keys.at[kv], keys.at[2 + kv], bias, s_ref, m_ref, l_ref, acc_ref
        )

        @pl.when(t < 4)
        def _():
            z_send(t + 4)

        @pl.when((t < 6) & (t != 2))
        def _():
            x_send(t + 2 - t // 3)

        @pl.when(t == 3)
        def _():
            for rel in (3, 2):
                for kv in range(2):
                    for g in range(GROUP):
                        o_copy(kv, g, rel).start()

        @pl.when((t == 4) | (t == 5))
        def _():
            for g in range(GROUP):
                o_copy(kv, g, 1).start()

        @pl.when(t >= 6)
        def _():
            for g in range(GROUP):
                attended[:, head_cols((kv * 4 + chunk) * GROUP + g)] = obuf[kv, chunk, pl.ds(g * 256, 256)]

        @pl.when(t == 4)
        def _():
            for rel in (3, 2, 1):
                for frm in range(4):
                    l_copy(frm, rel).start()
            for frm in range(4):
                out[0, :, head_cols(frm * 4 + chunk)] = keys[frm, x, zh, half_rows(core)]

        @pl.when(t == 7)
        def _():
            x_send(7)

    @pl.loop(0, ROUNDS)
    def _(u):
        for step in others:
            y_copy(0, step, u).wait_send()
            when_is(lax.rem(x + step, 4), range(4), lambda v: g_copy(u, step, v + 1).wait_send())
        z0_copy(u, 1).wait_send()

    for kv in range(2):
        for g in range(GROUP):
            for rel in (1, 2, 3):
                q_copy(kv, g, rel).wait_send()
                o_copy(kv, g, rel).wait()

    for frm in range(4):
        for rel in (1, 2, 3):
            l_copy(frm, rel).wait()

    @pl.loop(1, LAYERS)
    def _(layer):
        for step in others:
            y_copy(layer, step).wait_send()
        for step, flip in zorder:
            if step * 2 + flip:
                z_copy(layer, step, flip).wait_send()
        for piece in range(4):
            for step in others:
                x_copy(layer, step, piece).wait()


def relay(cache, queries, counts, blocks):
    dma = pltpu.SemaphoreType.DMA
    bf = jnp.bfloat16
    f32 = jnp.float32
    rows = GROUP * 256
    anyspace = pl.BlockSpec(memory_space=pl.ANY)
    sems = [
        (4, 3), (4, 3), (4,), (7, 3), (7, 3), (7,), (4,), (4,), (4,), (7, 8), (7, 8), (4, 3), (4, 3),
        (7, 3, 4), (7, 3, 4), (4, 4), (4, 4), (2, 4, 4), (2, 4, 4), (2, 4, 4), (2, 4, 4), (2,),
    ]
    return pl.pallas_call(
        relay_kernel,
        out_shape=(
            jax.ShapeDtypeStruct((LAYERS, 256, 2048), bf),
            jax.ShapeDtypeStruct((256, QH * HD), bf),
            jax.ShapeDtypeStruct((LAYERS, 2, 2, 2, SEQD, HD), bf),
        ),
        in_specs=[anyspace] * 4,
        out_specs=(pl.BlockSpec(memory_space=pltpu.VMEM),) * 2 + (anyspace,),
        scratch_shapes=[
            pltpu.VMEM((8, SEQD), f32),
            pltpu.SMEM((64,), jnp.int32),
            pltpu.SMEM((64, SECTIONS), jnp.int32),
            pltpu.VMEM((4, 4, 2, SEQD, HD), bf),
            pltpu.VMEM((LAYERS - 1, 4, 4, 256, HD), bf),
            pltpu.VMEM((2, 4, rows, HD), bf),
            pltpu.VMEM((2, 4, rows, HD), bf),
            pltpu.VMEM((8, rows, SEQD), f32),
            pltpu.VMEM((rows, 128), f32),
            pltpu.VMEM((rows, 128), f32),
            pltpu.VMEM((rows, HD), f32),
        ]
        + [dma(shape) for shape in sems],
        compiler_params=pltpu.CompilerParams(collective_id=0, has_side_effects=True, vmem_limit_bytes=40 << 20),
    )(cache.reshape(LAYERS, 2, 2, 2, SEQD, HD), queries, counts, blocks)


def settle_kernel(out, attended, out_to, attended_to, sems):
    copies = [pltpu.make_async_copy(out.at[layer], out_to.at[layer], sems.at[layer]) for layer in range(LAYERS)]
    copies.append(pltpu.make_async_copy(attended, attended_to, sems.at[LAYERS]))
    for copy in copies:
        copy.start()
    for copy in copies:
        copy.wait()


def settle(out, attended):
    vmem, anyspace = pl.BlockSpec(memory_space=pltpu.VMEM), pl.BlockSpec(memory_space=pl.ANY)
    return pl.pallas_call(
        settle_kernel,
        out_shape=tuple(jax.ShapeDtypeStruct(a.shape, a.dtype) for a in (out, attended)),
        in_specs=[vmem, vmem],
        out_specs=(anyspace, anyspace),
        scratch_shapes=[pltpu.SemaphoreType.DMA((LAYERS + 1,))],
        compiler_params=pltpu.CompilerParams(vmem_limit_bytes=16 << 20),
    )(out, attended)


def local(summary_cache, queries, section_counts, summary_blocks):
    relayed, attended, _ = relay(summary_cache, queries[0], section_counts, summary_blocks)
    relayed, attended = settle(relayed, attended)
    return attended[None], relayed[:, None]


def solution(mesh):
    placed = (P(None, "doc", None, "ctx"), P("doc", "ctx", None), P(), P())
    return jax.shard_map(
        local,
        mesh=mesh,
        in_specs=placed,
        out_specs=(P("doc", "ctx", None), P(None, "doc", "ctx", None)),
        check_vma=False,
    )
```

```python
import functools
import math

import jax
import jax.numpy as jnp
from jax import lax
from jax.experimental import pallas as pl
from jax.experimental.pallas import tpu as pltpu
from jax.sharding import PartitionSpec as P

QH = 32
KVH = 8
HD = 128
BLOCK = 128
SECTIONS = 2
GROUP = 4
SUMLEN = 256
SEQD = 512
LAYERS = 8
GSEQ = 4096
CHUNKS = 16
NEGATIVE = -1e30
MESH = pl.DeviceIdType.MESH
SCALE = (1.0 / math.sqrt(HD)) * math.log2(math.e)


def place(x, y, z, core):
    return (lax.rem(z, 2) * 4 + y, x * 4 + (z // 2) * 2 + core)


def head_group(mine, half, q_ref, k_ref, v_ref, bias_ref, s_ref, m_ref, l_ref, acc_ref):
    rows = q_ref.shape[0]

    def score(doc, diagonal):
        k = k_ref[doc // 2, lax.rem(doc, 2)]
        s = lax.dot_general(q_ref[...], k, (((1,), (1,)), ((), ())), preferred_element_type=jnp.float32)
        s = s * SCALE + bias_ref[pl.ds(doc, 1), :]
        if diagonal:
            at = lax.rem(lax.broadcasted_iota(jnp.int32, s.shape, 0), 256) + half * 256
            s = jnp.where(lax.broadcasted_iota(jnp.int32, s.shape, 1) <= at, s, NEGATIVE)
        s_ref[doc] = s
        top = jnp.maximum(jnp.maximum(s[:, 0:128], s[:, 128:256]), jnp.maximum(s[:, 256:384], s[:, 384:512]))
        return top

    def weigh(doc):
        v = v_ref[doc // 2, lax.rem(doc, 2)]
        top = m_ref[...]
        w = [jnp.exp2(s_ref[doc, :, i * 128 : (i + 1) * 128] - top) for i in range(4)]
        part = (w[0] + w[1]) + (w[2] + w[3])
        pair = [jnp.concatenate([w[2 * i].astype(jnp.bfloat16), w[2 * i + 1].astype(jnp.bfloat16)], axis=1) for i in range(2)]
        summed = lax.dot_general(
            jnp.concatenate(pair, axis=1), v, (((1,), (0,)), ((), ())), preferred_element_type=jnp.float32
        )
        return part, summed

    m_ref[...] = score(mine, True)

    @pl.loop(0, mine)
    def _(doc):
        m_ref[...] = jnp.maximum(m_ref[...], score(doc, False))

    m_ref[...] = jnp.broadcast_to(jnp.max(m_ref[...], axis=1, keepdims=True), m_ref.shape)
    part, summed = weigh(mine)
    l_ref[...] = part
    acc_ref[...] = summed

    @pl.loop(0, mine)
    def _(doc):
        part, summed = weigh(doc)
        l_ref[...] += part
        acc_ref[...] += summed

    return (acc_ref[...] / jnp.sum(l_ref[...], axis=1, keepdims=True)).astype(jnp.bfloat16)


ROUNDS = 4
PART = SEQD // ROUNDS


def relay_kernel(
    cache, queries, counts_hbm, blocks_hbm, out, attended, ybuf, bias, counts, blocks, keys, zbuf, qbuf, obuf, s_ref, m_ref, l_ref, acc_ref,
    y0s, y0r, y0o, ys, yr, yo, z0s, z0r, z0o, zs, zr, gs, gr, xs, xr, ls, lr, qs, qr, os, rs, cs,
):
    d = lax.axis_index("doc")
    c = lax.axis_index("ctx")
    zl, y = d // 4, lax.rem(d, 4)
    x, zh, core = c // 4, lax.rem(c // 2, 2), lax.rem(c, 2)
    z = zh * 2 + zl
    chunk = zh * 2 + core
    others = (1, 3, 2)

    def remote(src, dst, ssem, rsem, dev):
        return pltpu.make_async_remote_copy(src, dst, ssem, rsem, device_id=dev, device_id_type=MESH)

    def when_is(value, options, body):
        for v in options:
            @pl.when(value == v)
            def _():
                body(v)

    def part(u):
        return pl.ds(pl.multiple_of(u * PART, PART), PART)

    def half_rows(half):
        return pl.ds(pl.multiple_of(half * 256, 256), 256)

    def head_cols(h):
        return pl.ds(pl.multiple_of(h * HD, HD), HD)

    def y_copy(layer, step, u=None):
        to = lax.rem(y + step, 4)
        src = cache.at[layer, :, to // 2, lax.rem(to, 2)]
        dst = ybuf.at[layer, y // 2, lax.rem(y, 2)]
        if u is None:
            ssem, rsem, own, at = ys, yr, yo, layer - 1
        else:
            ssem, rsem, own, at = y0s, y0r, y0o, u
            src, dst = src.at[:, part(u)], dst.at[:, part(u)]
        if step == 0:
            return pltpu.make_async_copy(src, dst, own.at[at])
        return remote(src, dst, ssem.at[at, step - 1], rsem.at[at, step - 1], place(x, to, z, core))

    def y_wait(layer, u=None):
        for step in others:
            y_copy(layer, step, u).wait_recv()
        y_copy(layer, 0, u).wait()

    def z0_copy(u, flip):
        to = lax.rem(zl + flip, 2)
        src = ybuf.at[0, :, :, to, part(u)]
        dst = keys.at[x, pl.ds(zl * 2, 2), :, part(u)]
        if flip == 0:
            return pltpu.make_async_copy(src, dst, z0o.at[u])
        return remote(src, dst, z0s.at[u], z0r.at[u], place(x, y, zh * 2 + to, core))

    def g_copy(u, step, n):
        to = lax.rem(x + step, 4)
        ref = keys.at[x, pl.ds(0, n), :, part(u)]
        return remote(ref, ref, gs.at[u, step - 1], gr.at[u, step - 1], place(to, y, z, core))

    def peer(rel):
        return lax.rem(zh + rel // 2, 2), lax.rem(core + lax.rem(rel, 2), 2)

    def peer_place(rel):
        to_zh, to_core = peer(rel)
        return place(x, y, to_zh * 2 + zl, to_core)

    def l_copy(frm, rel):
        to_zh, to_core = peer(rel)
        src = keys.at[frm, x, to_zh, half_rows(to_core)]
        dst = out.at[0, :, head_cols(frm * 4 + chunk)]
        return remote(src, dst, ls.at[frm, rel], lr.at[frm, rel], peer_place(rel))

    def q_copy(kv, g, rel):
        to_zh, to_core = peer(rel)
        src = queries.at[:, head_cols((kv * 4 + to_zh * 2 + to_core) * GROUP + g)]
        dst = qbuf.at[kv, chunk, pl.ds(g * 256, 256)]
        if rel == 0:
            return pltpu.make_async_copy(src, dst, qr.at[kv, g, 0])
        return remote(src, dst, qs.at[kv, g, rel], qr.at[kv, g, rel], peer_place(rel))

    def o_copy(kv, g, rel):
        to_zh, to_core = peer(rel)
        src = obuf.at[kv, to_zh * 2 + to_core, pl.ds(g * 256, 256)]
        dst = attended.at[:, head_cols((kv * 4 + chunk) * GROUP + g)]
        return remote(src, dst, os.at[kv, g, rel], rs.at[kv, g, rel], peer_place(rel))

    zorder = ((1, 0), (1, 1), (3, 0), (3, 1), (2, 0), (2, 1), (0, 1), (0, 0))

    def z_copy(layer, step, flip):
        to_z, to_core = lax.rem(z + step, 4), lax.rem(core + flip, 2)
        r = step * 2 + flip
        src = ybuf.at[layer, :, to_z // 2, lax.rem(to_z, 2), half_rows(to_core)]
        dst = zbuf.at[layer - 1, pl.ds(zl * 2, 2), chunk]
        if r == 0:
            return pltpu.make_async_copy(src, dst, zr.at[layer - 1, 0])
        return remote(src, dst, zs.at[layer - 1, r], zr.at[layer - 1, r], place(x, y, to_z, to_core))

    def x_copy(layer, step, piece):
        to = lax.rem(x + step, 4)
        src = zbuf.at[layer - 1, to, piece]
        dst = out.at[layer, :, head_cols(x * 4 + piece)]
        return remote(src, dst, xs.at[layer - 1, step - 1, piece], xr.at[layer - 1, step - 1, piece], place(to, y, z, core))

    def z_send(layer):
        y_wait(layer)
        for step, flip in zorder:
            z_copy(layer, step, flip).start()

    def x_send(layer):
        for step, flip in zorder:
            if step * 2 + flip == 0:
                z_copy(layer, 0, 0).wait()
            else:
                z_copy(layer, step, flip).wait_recv()
        for step in others:
            for piece in range(4):
                x_copy(layer, step, piece).start()
        for piece in range(4):
            out[layer, :, head_cols(x * 4 + piece)] = zbuf[layer - 1, x, piece]

    barrier = pltpu.get_barrier_semaphore()
    peers = [place(x, lax.rem(y + step, 4), z, core) for step in others]
    peers += [place(lax.rem(x + step, 4), y, z, core) for step in others]
    peers += [place(x, y, lax.rem(z + step, 4), lax.rem(core + flip, 2)) for step, flip in zorder if step or flip]
    for peer_device in peers:
        pl.semaphore_signal(barrier, inc=1, device_id=peer_device, device_id_type=MESH)
    tables = [pltpu.make_async_copy(counts_hbm, counts, cs.at[0]), pltpu.make_async_copy(blocks_hbm, blocks, cs.at[1])]
    for copy in tables:
        copy.start()
    for u in range(ROUNDS):
        y_copy(0, 0, u).start()
    pl.semaphore_wait(barrier, len(peers))

    @pl.loop(0, ROUNDS)
    def _(u):
        for step in others:
            y_copy(0, step, u).start()

    @pl.loop(1, LAYERS)
    def _(layer):
        for step in others + (0,):
            y_copy(layer, step).start()

    def q_send(kv, g):
        for rel in (3, 2, 1, 0):
            q_copy(kv, g, rel).start()

    for g in range(2):
        q_send(0, g)

    @pl.loop(0, ROUNDS + 1)
    def _(t):
        @pl.when(t < ROUNDS)
        def _():
            y_wait(0, t)
            z0_copy(t, 1).start()
            z0_copy(t, 0).start()

        @pl.when(t >= 1)
        def _():
            z0_copy(t - 1, 1).wait_recv()
            z0_copy(t - 1, 0).wait()
            for step in others:
                when_is(lax.rem(x + step, 4), range(4), lambda v: g_copy(t - 1, step, v + 1).start())

        when_is(t, range(2), lambda v: q_send(0, 2 + v))
        when_is(t, range(2, 4), lambda v: q_send(1, v - 2))

    for g in range(2, GROUP):
        q_send(1, g)

    for copy in tables:
        copy.wait()
    slot = lax.broadcasted_iota(jnp.int32, (1, SEQD), 1)
    second = slot // SUMLEN
    for doc in range(8):
        at = doc * 8 + d
        live_blocks = jnp.where(second == 0, blocks[at, 0], blocks[at, 1])
        live = (second < counts[at]) & (slot - second * SUMLEN < BLOCK * live_blocks)
        bias[doc : doc + 1, :] = jnp.where(live, 0.0, NEGATIVE)

    @pl.loop(1, 5)
    def _(layer):
        z_send(layer)

    def gathered(v):
        @pl.loop(0, ROUNDS)
        def _(u):
            for step in others:
                g_copy(u, step, v + 1).wait_recv()

    when_is(x, range(4), gathered)
    x_send(1)

    @pl.loop(0, 8)
    def _(t):
        rel = 3 - t // 2
        kv = lax.rem(t, 2)
        to_zh, to_core = peer(rel)
        for g in range(GROUP):
            pltpu.make_async_copy(queries.at[:, head_cols(g)], qbuf.at[kv, 0, pl.ds(g * 256, 256)], qr.at[kv, g, rel]).wait()
        src = to_zh * 2 + to_core
        obuf[kv, src] = head_group(
            x * 2 + to_zh, to_core, qbuf.at[kv, src], keys.at[kv], keys.at[2 + kv], bias, s_ref, m_ref, l_ref, acc_ref
        )

        @pl.when((t == 0) | (t == 2) | (t == 3))
        def _():
            z_send(t - t // 2 + 5)
            x_send(t - t // 2 + 2)

        @pl.when((t == 4) | (t == 5))
        def _():
            x_send(t + 1)

        @pl.when(t == 3)
        def _():
            for rel in (3, 2):
                for kv in range(2):
                    for g in range(GROUP):
                        o_copy(kv, g, rel).start()

        @pl.when((t == 4) | (t == 5))
        def _():
            for g in range(GROUP):
                o_copy(kv, g, 1).start()

        @pl.when(t >= 6)
        def _():
            for g in range(GROUP):
                attended[:, head_cols((kv * 4 + chunk) * GROUP + g)] = obuf[kv, chunk, pl.ds(g * 256, 256)]

        @pl.when(t == 4)
        def _():
            for rel in (3, 2, 1):
                for frm in range(4):
                    l_copy(frm, rel).start()
            for frm in range(4):
                out[0, :, head_cols(frm * 4 + chunk)] = keys[frm, x, zh, half_rows(core)]

        @pl.when(t == 7)
        def _():
            x_send(7)

    @pl.loop(0, ROUNDS)
    def _(u):
        for step in others:
            y_copy(0, step, u).wait_send()
            when_is(lax.rem(x + step, 4), range(4), lambda v: g_copy(u, step, v + 1).wait_send())
        z0_copy(u, 1).wait_send()

    for kv in range(2):
        for g in range(GROUP):
            for rel in (1, 2, 3):
                q_copy(kv, g, rel).wait_send()
                o_copy(kv, g, rel).wait()

    for frm in range(4):
        for rel in (1, 2, 3):
            l_copy(frm, rel).wait()

    @pl.loop(1, LAYERS)
    def _(layer):
        for step in others:
            y_copy(layer, step).wait_send()
        for step, flip in zorder:
            if step * 2 + flip:
                z_copy(layer, step, flip).wait_send()
        for piece in range(4):
            for step in others:
                x_copy(layer, step, piece).wait()


def relay(cache, queries, counts, blocks):
    dma = pltpu.SemaphoreType.DMA
    bf = jnp.bfloat16
    f32 = jnp.float32
    rows = GROUP * 256
    anyspace = pl.BlockSpec(memory_space=pl.ANY)
    sems = [
        (4, 3), (4, 3), (4,), (7, 3), (7, 3), (7,), (4,), (4,), (4,), (7, 8), (7, 8), (4, 3), (4, 3),
        (7, 3, 4), (7, 3, 4), (4, 4), (4, 4), (2, 4, 4), (2, 4, 4), (2, 4, 4), (2, 4, 4), (2,),
    ]
    return pl.pallas_call(
        relay_kernel,
        out_shape=(
            jax.ShapeDtypeStruct((LAYERS, 256, 2048), bf),
            jax.ShapeDtypeStruct((256, QH * HD), bf),
            jax.ShapeDtypeStruct((LAYERS, 2, 2, 2, SEQD, HD), bf),
        ),
        in_specs=[anyspace] * 4,
        out_specs=(pl.BlockSpec(memory_space=pltpu.VMEM),) * 2 + (anyspace,),
        scratch_shapes=[
            pltpu.VMEM((8, SEQD), f32),
            pltpu.SMEM((64,), jnp.int32),
            pltpu.SMEM((64, SECTIONS), jnp.int32),
            pltpu.VMEM((4, 4, 2, SEQD, HD), bf),
            pltpu.VMEM((LAYERS - 1, 4, 4, 256, HD), bf),
            pltpu.VMEM((2, 4, rows, HD), bf),
            pltpu.VMEM((2, 4, rows, HD), bf),
            pltpu.VMEM((8, rows, SEQD), f32),
            pltpu.VMEM((rows, 128), f32),
            pltpu.VMEM((rows, 128), f32),
            pltpu.VMEM((rows, HD), f32),
        ]
        + [dma(shape) for shape in sems],
        compiler_params=pltpu.CompilerParams(collective_id=0, has_side_effects=True, vmem_limit_bytes=40 << 20),
    )(cache.reshape(LAYERS, 2, 2, 2, SEQD, HD), queries, counts, blocks)


def settle_kernel(out, attended, out_to, attended_to, sems):
    copies = [pltpu.make_async_copy(out.at[layer], out_to.at[layer], sems.at[layer]) for layer in range(LAYERS)]
    copies.append(pltpu.make_async_copy(attended, attended_to, sems.at[LAYERS]))
    for copy in copies:
        copy.start()
    for copy in copies:
        copy.wait()


def settle(out, attended):
    vmem, anyspace = pl.BlockSpec(memory_space=pltpu.VMEM), pl.BlockSpec(memory_space=pl.ANY)
    return pl.pallas_call(
        settle_kernel,
        out_shape=tuple(jax.ShapeDtypeStruct(a.shape, a.dtype) for a in (out, attended)),
        in_specs=[vmem, vmem],
        out_specs=(anyspace, anyspace),
        scratch_shapes=[pltpu.SemaphoreType.DMA((LAYERS + 1,))],
        compiler_params=pltpu.CompilerParams(vmem_limit_bytes=16 << 20),
    )(out, attended)


def local(summary_cache, queries, section_counts, summary_blocks):
    relayed, attended, _ = relay(summary_cache, queries[0], section_counts, summary_blocks)
    relayed, attended = settle(relayed, attended)
    return attended[None], relayed[:, None]


def solution(mesh):
    placed = (P(None, "doc", None, "ctx"), P("doc", "ctx", None), P(), P())
    return jax.shard_map(
        local,
        mesh=mesh,
        in_specs=placed,
        out_specs=(P("doc", "ctx", None), P(None, "doc", "ctx", None)),
        check_vma=False,
    )
```

```python
import functools
import math

import jax
import jax.numpy as jnp
from jax import lax
from jax.experimental import pallas as pl
from jax.experimental.pallas import tpu as pltpu
from jax.sharding import PartitionSpec as P

QH = 32
KVH = 8
HD = 128
BLOCK = 128
SECTIONS = 2
GROUP = 4
SUMLEN = 256
SEQD = 512
LAYERS = 8
GSEQ = 4096
CHUNKS = 16
NEGATIVE = -1e30
MESH = pl.DeviceIdType.MESH
SCALE = (1.0 / math.sqrt(HD)) * math.log2(math.e)


def place(x, y, z, core):
    return (lax.rem(z, 2) * 4 + y, x * 4 + (z // 2) * 2 + core)


def head_group(mine, half, q_ref, k_ref, v_ref, bias_ref, s_ref, m_ref, l_ref, acc_ref):
    rows = q_ref.shape[0]

    def score(doc, diagonal):
        k = k_ref[doc // 2, lax.rem(doc, 2)]
        s = lax.dot_general(q_ref[...], k, (((1,), (1,)), ((), ())), preferred_element_type=jnp.float32)
        s = s * SCALE + bias_ref[pl.ds(doc, 1), :]
        if diagonal:
            at = lax.rem(lax.broadcasted_iota(jnp.int32, s.shape, 0), 256) + half * 256
            s = jnp.where(lax.broadcasted_iota(jnp.int32, s.shape, 1) <= at, s, NEGATIVE)
        s_ref[doc] = s
        top = jnp.maximum(jnp.maximum(s[:, 0:128], s[:, 128:256]), jnp.maximum(s[:, 256:384], s[:, 384:512]))
        return top

    def weigh(doc):
        v = v_ref[doc // 2, lax.rem(doc, 2)]
        top = m_ref[...]
        w = [jnp.exp2(s_ref[doc, :, i * 128 : (i + 1) * 128] - top) for i in range(4)]
        part = (w[0] + w[1]) + (w[2] + w[3])
        pair = [jnp.concatenate([w[2 * i].astype(jnp.bfloat16), w[2 * i + 1].astype(jnp.bfloat16)], axis=1) for i in range(2)]
        summed = lax.dot_general(
            jnp.concatenate(pair, axis=1), v, (((1,), (0,)), ((), ())), preferred_element_type=jnp.float32
        )
        return part, summed

    m_ref[...] = score(mine, True)

    @pl.loop(0, mine)
    def _(doc):
        m_ref[...] = jnp.maximum(m_ref[...], score(doc, False))

    m_ref[...] = jnp.broadcast_to(jnp.max(m_ref[...], axis=1, keepdims=True), m_ref.shape)
    part, summed = weigh(mine)
    l_ref[...] = part
    acc_ref[...] = summed

    @pl.loop(0, mine)
    def _(doc):
        part, summed = weigh(doc)
        l_ref[...] += part
        acc_ref[...] += summed

    return (acc_ref[...] / jnp.sum(l_ref[...], axis=1, keepdims=True)).astype(jnp.bfloat16)


ROUNDS = 4
PART = SEQD // ROUNDS


def relay_kernel(
    cache, queries, counts_hbm, blocks_hbm, out, attended, ybuf, bias, counts, blocks, keys, zbuf, qbuf, obuf, s_ref, m_ref, l_ref, acc_ref,
    y0s, y0r, y0o, ys, yr, yo, z0s, z0r, z0o, zs, zr, gs, gr, xs, xr, ls, lr, qs, qr, os, rs, cs,
):
    d = lax.axis_index("doc")
    c = lax.axis_index("ctx")
    zl, y = d // 4, lax.rem(d, 4)
    x, zh, core = c // 4, lax.rem(c // 2, 2), lax.rem(c, 2)
    z = zh * 2 + zl
    chunk = zh * 2 + core
    others = (1, 3, 2)

    def remote(src, dst, ssem, rsem, dev):
        return pltpu.make_async_remote_copy(src, dst, ssem, rsem, device_id=dev, device_id_type=MESH)

    def when_is(value, options, body):
        for v in options:
            @pl.when(value == v)
            def _():
                body(v)

    def part(u):
        return pl.ds(pl.multiple_of(u * PART, PART), PART)

    def half_rows(half):
        return pl.ds(pl.multiple_of(half * 256, 256), 256)

    def head_cols(h):
        return pl.ds(pl.multiple_of(h * HD, HD), HD)

    def y_copy(layer, step, u=None):
        to = lax.rem(y + step, 4)
        src = cache.at[layer, :, to // 2, lax.rem(to, 2)]
        dst = ybuf.at[layer, y // 2, lax.rem(y, 2)]
        if u is None:
            ssem, rsem, own, at = ys, yr, yo, layer - 1
        else:
            ssem, rsem, own, at = y0s, y0r, y0o, u
            src, dst = src.at[:, part(u)], dst.at[:, part(u)]
        if step == 0:
            return pltpu.make_async_copy(src, dst, own.at[at])
        return remote(src, dst, ssem.at[at, step - 1], rsem.at[at, step - 1], place(x, to, z, core))

    def y_wait(layer, u=None):
        for step in others:
            y_copy(layer, step, u).wait_recv()
        y_copy(layer, 0, u).wait()

    def z0_copy(u, flip):
        to = lax.rem(zl + flip, 2)
        src = ybuf.at[0, :, :, to, part(u)]
        dst = keys.at[x, pl.ds(zl * 2, 2), :, part(u)]
        if flip == 0:
            return pltpu.make_async_copy(src, dst, z0o.at[u])
        return remote(src, dst, z0s.at[u], z0r.at[u], place(x, y, zh * 2 + to, core))

    def g_copy(u, step, n):
        to = lax.rem(x + step, 4)
        ref = keys.at[x, pl.ds(0, n), :, part(u)]
        return remote(ref, ref, gs.at[u, step - 1], gr.at[u, step - 1], place(to, y, z, core))

    def peer(rel):
        return lax.rem(zh + rel // 2, 2), lax.rem(core + lax.rem(rel, 2), 2)

    def peer_place(rel):
        to_zh, to_core = peer(rel)
        return place(x, y, to_zh * 2 + zl, to_core)

    def l_copy(frm, rel):
        to_zh, to_core = peer(rel)
        src = keys.at[frm, x, to_zh, half_rows(to_core)]
        dst = out.at[0, :, head_cols(frm * 4 + chunk)]
        return remote(src, dst, ls.at[frm, rel], lr.at[frm, rel], peer_place(rel))

    def q_copy(kv, g, rel):
        to_zh, to_core = peer(rel)
        src = queries.at[:, head_cols((kv * 4 + to_zh * 2 + to_core) * GROUP + g)]
        dst = qbuf.at[kv, chunk, pl.ds(g * 256, 256)]
        if rel == 0:
            return pltpu.make_async_copy(src, dst, qr.at[kv, g, 0])
        return remote(src, dst, qs.at[kv, g, rel], qr.at[kv, g, rel], peer_place(rel))

    def o_copy(kv, g, rel):
        to_zh, to_core = peer(rel)
        src = obuf.at[kv, to_zh * 2 + to_core, pl.ds(g * 256, 256)]
        dst = attended.at[:, head_cols((kv * 4 + chunk) * GROUP + g)]
        return remote(src, dst, os.at[kv, g, rel], rs.at[kv, g, rel], peer_place(rel))

    zorder = ((1, 0), (1, 1), (3, 0), (3, 1), (2, 0), (2, 1), (0, 1), (0, 0))

    def z_copy(layer, step, flip):
        to_z, to_core = lax.rem(z + step, 4), lax.rem(core + flip, 2)
        r = step * 2 + flip
        src = ybuf.at[layer, :, to_z // 2, lax.rem(to_z, 2), half_rows(to_core)]
        dst = zbuf.at[layer - 1, pl.ds(zl * 2, 2), chunk]
        if r == 0:
            return pltpu.make_async_copy(src, dst, zr.at[layer - 1, 0])
        return remote(src, dst, zs.at[layer - 1, r], zr.at[layer - 1, r], place(x, y, to_z, to_core))

    def x_copy(layer, step, piece):
        to = lax.rem(x + step, 4)
        src = zbuf.at[layer - 1, to, piece]
        dst = out.at[layer, :, head_cols(x * 4 + piece)]
        return remote(src, dst, xs.at[layer - 1, step - 1, piece], xr.at[layer - 1, step - 1, piece], place(to, y, z, core))

    def z_send(layer):
        y_wait(layer)
        for step, flip in zorder:
            z_copy(layer, step, flip).start()

    def x_send(layer):
        for step, flip in zorder:
            if step * 2 + flip == 0:
                z_copy(layer, 0, 0).wait()
            else:
                z_copy(layer, step, flip).wait_recv()
        for step in others:
            for piece in range(4):
                x_copy(layer, step, piece).start()
        for piece in range(4):
            out[layer, :, head_cols(x * 4 + piece)] = zbuf[layer - 1, x, piece]

    barrier = pltpu.get_barrier_semaphore()
    peers = [place(x, lax.rem(y + step, 4), z, core) for step in others]
    peers += [place(lax.rem(x + step, 4), y, z, core) for step in others]
    peers += [place(x, y, lax.rem(z + step, 4), lax.rem(core + flip, 2)) for step, flip in zorder if step or flip]
    for peer_device in peers:
        pl.semaphore_signal(barrier, inc=1, device_id=peer_device, device_id_type=MESH)
    tables = [pltpu.make_async_copy(counts_hbm, counts, cs.at[0]), pltpu.make_async_copy(blocks_hbm, blocks, cs.at[1])]
    for copy in tables:
        copy.start()
    for u in range(ROUNDS):
        y_copy(0, 0, u).start()
    pl.semaphore_wait(barrier, len(peers))

    @pl.loop(0, ROUNDS)
    def _(u):
        for step in others:
            y_copy(0, step, u).start()

    @pl.loop(1, LAYERS)
    def _(layer):
        for step in others + (0,):
            y_copy(layer, step).start()

    def q_send(kv, g):
        for rel in (3, 2, 1, 0):
            q_copy(kv, g, rel).start()

    for g in range(2):
        q_send(0, g)

    @pl.loop(0, ROUNDS + 1)
    def _(t):
        @pl.when(t < ROUNDS)
        def _():
            y_wait(0, t)
            z0_copy(t, 1).start()
            z0_copy(t, 0).start()

        @pl.when(t >= 1)
        def _():
            z0_copy(t - 1, 1).wait_recv()
            z0_copy(t - 1, 0).wait()
            for step in others:
                when_is(lax.rem(x + step, 4), range(4), lambda v: g_copy(t - 1, step, v + 1).start())

        when_is(t, range(2), lambda v: q_send(0, 2 + v))
        when_is(t, range(2, 4), lambda v: q_send(1, v - 2))

    for g in range(2, GROUP):
        q_send(1, g)

    for copy in tables:
        copy.wait()
    slot = lax.broadcasted_iota(jnp.int32, (1, SEQD), 1)
    second = slot // SUMLEN
    for doc in range(8):
        at = doc * 8 + d
        live_blocks = jnp.where(second == 0, blocks[0, at], blocks[1, at])
        live = (second < counts[at]) & (slot - second * SUMLEN < BLOCK * live_blocks)
        bias[doc : doc + 1, :] = jnp.where(live, 0.0, NEGATIVE)

    @pl.loop(1, 5)
    def _(layer):
        z_send(layer)

    def gathered(v):
        @pl.loop(0, ROUNDS)
        def _(u):
            for step in others:
                g_copy(u, step, v + 1).wait_recv()

    when_is(x, range(4), gathered)
    x_send(1)

    @pl.loop(0, 8)
    def _(t):
        rel = 3 - t // 2
        kv = lax.rem(t, 2)
        to_zh, to_core = peer(rel)
        for g in range(GROUP):
            pltpu.make_async_copy(queries.at[:, head_cols(g)], qbuf.at[kv, 0, pl.ds(g * 256, 256)], qr.at[kv, g, rel]).wait()
        src = to_zh * 2 + to_core
        obuf[kv, src] = head_group(
            x * 2 + to_zh, to_core, qbuf.at[kv, src], keys.at[kv], keys.at[2 + kv], bias, s_ref, m_ref, l_ref, acc_ref
        )

        @pl.when((t == 0) | (t == 2) | (t == 3))
        def _():
            z_send(t - t // 2 + 5)
            x_send(t - t // 2 + 2)

        @pl.when((t == 4) | (t == 5))
        def _():
            x_send(t + 1)

        @pl.when(t == 3)
        def _():
            for rel in (3, 2):
                for kv in range(2):
                    for g in range(GROUP):
                        o_copy(kv, g, rel).start()

        @pl.when((t == 4) | (t == 5))
        def _():
            for g in range(GROUP):
                o_copy(kv, g, 1).start()

        @pl.when(t >= 6)
        def _():
            for g in range(GROUP):
                attended[:, head_cols((kv * 4 + chunk) * GROUP + g)] = obuf[kv, chunk, pl.ds(g * 256, 256)]

        @pl.when(t == 4)
        def _():
            for rel in (3, 2, 1):
                for frm in range(4):
                    l_copy(frm, rel).start()
            for frm in range(4):
                out[0, :, head_cols(frm * 4 + chunk)] = keys[frm, x, zh, half_rows(core)]

        @pl.when(t == 7)
        def _():
            x_send(7)

    @pl.loop(0, ROUNDS)
    def _(u):
        for step in others:
            y_copy(0, step, u).wait_send()
            when_is(lax.rem(x + step, 4), range(4), lambda v: g_copy(u, step, v + 1).wait_send())
        z0_copy(u, 1).wait_send()

    for kv in range(2):
        for g in range(GROUP):
            for rel in (1, 2, 3):
                q_copy(kv, g, rel).wait_send()

    @pl.loop(1, LAYERS)
    def _(layer):
        for step in others:
            y_copy(layer, step).wait_send()
        for step, flip in zorder:
            if step * 2 + flip:
                z_copy(layer, step, flip).wait_send()
        for piece in range(4):
            for step in others:
                x_copy(layer, step, piece).wait()

    for kv in range(2):
        for g in range(GROUP):
            for rel in (1, 2, 3):
                o_copy(kv, g, rel).wait()

    for frm in range(4):
        for rel in (1, 2, 3):
            l_copy(frm, rel).wait()


def relay(cache, queries, counts, blocks):
    dma = pltpu.SemaphoreType.DMA
    bf = jnp.bfloat16
    f32 = jnp.float32
    rows = GROUP * 256
    anyspace = pl.BlockSpec(memory_space=pl.ANY)
    sems = [
        (4, 3), (4, 3), (4,), (7, 3), (7, 3), (7,), (4,), (4,), (4,), (7, 8), (7, 8), (4, 3), (4, 3),
        (7, 3, 4), (7, 3, 4), (4, 4), (4, 4), (2, 4, 4), (2, 4, 4), (2, 4, 4), (2, 4, 4), (2,),
    ]
    return pl.pallas_call(
        relay_kernel,
        out_shape=(
            jax.ShapeDtypeStruct((LAYERS, 256, 2048), bf),
            jax.ShapeDtypeStruct((256, QH * HD), bf),
            jax.ShapeDtypeStruct((LAYERS, 2, 2, 2, SEQD, HD), bf),
        ),
        in_specs=[anyspace] * 4,
        out_specs=(pl.BlockSpec(memory_space=pltpu.VMEM),) * 2 + (anyspace,),
        scratch_shapes=[
            pltpu.VMEM((8, SEQD), f32),
            pltpu.SMEM((64,), jnp.int32),
            pltpu.SMEM((SECTIONS, 64), jnp.int32),
            pltpu.VMEM((4, 4, 2, SEQD, HD), bf),
            pltpu.VMEM((LAYERS - 1, 4, 4, 256, HD), bf),
            pltpu.VMEM((2, 4, rows, HD), bf),
            pltpu.VMEM((2, 4, rows, HD), bf),
            pltpu.VMEM((8, rows, SEQD), f32),
            pltpu.VMEM((rows, 128), f32),
            pltpu.VMEM((rows, 128), f32),
            pltpu.VMEM((rows, HD), f32),
        ]
        + [dma(shape) for shape in sems],
        compiler_params=pltpu.CompilerParams(collective_id=0, has_side_effects=True, vmem_limit_bytes=40 << 20),
    )(cache.reshape(LAYERS, 2, 2, 2, SEQD, HD), *(pltpu.with_memory_space_constraint(a, pltpu.HBM) for a in (queries, counts, blocks.T)))


def settle_kernel(out, attended, out_to, attended_to, sems):
    copies = [pltpu.make_async_copy(out.at[layer], out_to.at[layer], sems.at[layer]) for layer in range(LAYERS)]
    copies.append(pltpu.make_async_copy(attended, attended_to, sems.at[LAYERS]))
    for copy in copies:
        copy.start()
    for copy in copies:
        copy.wait()


def settle(out, attended):
    vmem, anyspace = pl.BlockSpec(memory_space=pltpu.VMEM), pl.BlockSpec(memory_space=pl.ANY)
    return pl.pallas_call(
        settle_kernel,
        out_shape=tuple(jax.ShapeDtypeStruct(a.shape, a.dtype) for a in (out, attended)),
        in_specs=[vmem, vmem],
        out_specs=(anyspace, anyspace),
        scratch_shapes=[pltpu.SemaphoreType.DMA((LAYERS + 1,))],
        compiler_params=pltpu.CompilerParams(vmem_limit_bytes=16 << 20),
    )(out, attended)


def local(summary_cache, queries, section_counts, summary_blocks):
    relayed, attended, _ = relay(summary_cache, queries[0], section_counts, summary_blocks)
    relayed, attended = settle(relayed, attended)
    return attended[None], relayed[:, None]


def solution(mesh):
    placed = (P(None, "doc", None, "ctx"), P("doc", "ctx", None), P(), P())
    return jax.shard_map(
        local,
        mesh=mesh,
        in_specs=placed,
        out_specs=(P("doc", "ctx", None), P(None, "doc", "ctx", None)),
        check_vma=False,
    )
```

```python
import functools
import math

import jax
import jax.numpy as jnp
from jax import lax
from jax.experimental import pallas as pl
from jax.experimental.pallas import tpu as pltpu
from jax.sharding import PartitionSpec as P

QH = 32
KVH = 8
HD = 128
BLOCK = 128
SECTIONS = 2
GROUP = 4
SUMLEN = 256
SEQD = 512
LAYERS = 8
GSEQ = 4096
CHUNKS = 16
NEGATIVE = -1e30
MESH = pl.DeviceIdType.MESH
SCALE = (1.0 / math.sqrt(HD)) * math.log2(math.e)


def place(x, y, z, core):
    return (lax.rem(z, 2) * 4 + y, x * 4 + (z // 2) * 2 + core)


def head_group(mine, half, q_ref, k_ref, v_ref, bias_ref, s_ref, m_ref, l_ref, acc_ref):
    rows = q_ref.shape[0]

    def score(doc, diagonal):
        k = k_ref[doc // 2, lax.rem(doc, 2)]
        s = lax.dot_general(q_ref[...], k, (((1,), (1,)), ((), ())), preferred_element_type=jnp.float32)
        s = s * SCALE + bias_ref[pl.ds(doc, 1), :]
        if diagonal:
            at = lax.rem(lax.broadcasted_iota(jnp.int32, s.shape, 0), 256) + half * 256
            s = jnp.where(lax.broadcasted_iota(jnp.int32, s.shape, 1) <= at, s, NEGATIVE)
        s_ref[doc] = s
        top = jnp.maximum(jnp.maximum(s[:, 0:128], s[:, 128:256]), jnp.maximum(s[:, 256:384], s[:, 384:512]))
        return top

    def weigh(doc):
        v = v_ref[doc // 2, lax.rem(doc, 2)]
        top = m_ref[...]
        w = [jnp.exp2(s_ref[doc, :, i * 128 : (i + 1) * 128] - top) for i in range(4)]
        part = (w[0] + w[1]) + (w[2] + w[3])
        pair = [jnp.concatenate([w[2 * i].astype(jnp.bfloat16), w[2 * i + 1].astype(jnp.bfloat16)], axis=1) for i in range(2)]
        summed = lax.dot_general(
            jnp.concatenate(pair, axis=1), v, (((1,), (0,)), ((), ())), preferred_element_type=jnp.float32
        )
        return part, summed

    m_ref[...] = score(mine, True)

    @pl.loop(0, mine)
    def _(doc):
        m_ref[...] = jnp.maximum(m_ref[...], score(doc, False))

    m_ref[...] = jnp.broadcast_to(jnp.max(m_ref[...], axis=1, keepdims=True), m_ref.shape)
    part, summed = weigh(mine)
    l_ref[...] = part
    acc_ref[...] = summed

    @pl.loop(0, mine)
    def _(doc):
        part, summed = weigh(doc)
        l_ref[...] += part
        acc_ref[...] += summed

    return (acc_ref[...] / jnp.sum(l_ref[...], axis=1, keepdims=True)).astype(jnp.bfloat16)


ROUNDS = 4
PART = SEQD // ROUNDS


def relay_kernel(
    cache, queries, counts_hbm, blocks_hbm, out, attended, ybuf, bias, counts, blocks, keys, zbuf, qbuf, obuf, qstack, s_ref, m_ref, l_ref, acc_ref,
    y0s, y0r, y0o, ys, yr, yo, z0s, z0r, z0o, zs, zr, gs, gr, xs, xr, ls, lr, qs, qr, os, rs, cs,
):
    d = lax.axis_index("doc")
    c = lax.axis_index("ctx")
    zl, y = d // 4, lax.rem(d, 4)
    x, zh, core = c // 4, lax.rem(c // 2, 2), lax.rem(c, 2)
    z = zh * 2 + zl
    chunk = zh * 2 + core
    others = (1, 3, 2)

    def remote(src, dst, ssem, rsem, dev):
        return pltpu.make_async_remote_copy(src, dst, ssem, rsem, device_id=dev, device_id_type=MESH)

    def when_is(value, options, body):
        for v in options:
            @pl.when(value == v)
            def _():
                body(v)

    def part(u):
        return pl.ds(pl.multiple_of(u * PART, PART), PART)

    def half_rows(half):
        return pl.ds(pl.multiple_of(half * 256, 256), 256)

    def head_cols(h):
        return pl.ds(pl.multiple_of(h * HD, HD), HD)

    def y_copy(layer, step, u=None):
        to = lax.rem(y + step, 4)
        src = cache.at[layer, :, to // 2, lax.rem(to, 2)]
        dst = ybuf.at[layer, y // 2, lax.rem(y, 2)]
        if u is None:
            ssem, rsem, own, at = ys, yr, yo, layer - 1
        else:
            ssem, rsem, own, at = y0s, y0r, y0o, u
            src, dst = src.at[:, part(u)], dst.at[:, part(u)]
        if step == 0:
            return pltpu.make_async_copy(src, dst, own.at[at])
        return remote(src, dst, ssem.at[at, step - 1], rsem.at[at, step - 1], place(x, to, z, core))

    def y_wait(layer, u=None):
        for step in others:
            y_copy(layer, step, u).wait_recv()
        y_copy(layer, 0, u).wait()

    def z0_copy(u, flip):
        to = lax.rem(zl + flip, 2)
        src = ybuf.at[0, :, :, to, part(u)]
        dst = keys.at[x, pl.ds(zl * 2, 2), :, part(u)]
        if flip == 0:
            return pltpu.make_async_copy(src, dst, z0o.at[u])
        return remote(src, dst, z0s.at[u], z0r.at[u], place(x, y, zh * 2 + to, core))

    def g_copy(u, step, n):
        to = lax.rem(x + step, 4)
        ref = keys.at[x, pl.ds(0, n), :, part(u)]
        return remote(ref, ref, gs.at[u, step - 1], gr.at[u, step - 1], place(to, y, z, core))

    def peer(rel):
        return lax.rem(zh + rel // 2, 2), lax.rem(core + lax.rem(rel, 2), 2)

    def peer_place(rel):
        to_zh, to_core = peer(rel)
        return place(x, y, to_zh * 2 + zl, to_core)

    def l_copy(frm, rel):
        to_zh, to_core = peer(rel)
        src = keys.at[frm, x, to_zh, half_rows(to_core)]
        dst = out.at[0, :, head_cols(frm * 4 + chunk)]
        return remote(src, dst, ls.at[frm, rel], lr.at[frm, rel], peer_place(rel))

    def group_cols(k):
        return pl.ds(pl.multiple_of(k * GROUP * HD, GROUP * HD), GROUP * HD)

    def q_copy(kv, rel):
        to_zh, to_core = peer(rel)
        src = queries.at[:, group_cols(kv * 4 + to_zh * 2 + to_core)]
        dst = qbuf.at[kv, chunk]
        if rel == 0:
            return pltpu.make_async_copy(src, dst, qr.at[kv, 0])
        return remote(src, dst, qs.at[kv, rel], qr.at[kv, rel], peer_place(rel))

    def o_copy(kv, rel):
        to_zh, to_core = peer(rel)
        src = obuf.at[kv, to_zh * 2 + to_core]
        dst = attended.at[:, group_cols(kv * 4 + chunk)]
        return remote(src, dst, os.at[kv, rel], rs.at[kv, rel], peer_place(rel))

    zorder = ((1, 0), (1, 1), (3, 0), (3, 1), (2, 0), (2, 1), (0, 1), (0, 0))

    def z_copy(layer, step, flip):
        to_z, to_core = lax.rem(z + step, 4), lax.rem(core + flip, 2)
        r = step * 2 + flip
        src = ybuf.at[layer, :, to_z // 2, lax.rem(to_z, 2), half_rows(to_core)]
        dst = zbuf.at[layer - 1, pl.ds(zl * 2, 2), :, head_cols(chunk)]
        if r == 0:
            return pltpu.make_async_copy(src, dst, zr.at[layer - 1, 0])
        return remote(src, dst, zs.at[layer - 1, r], zr.at[layer - 1, r], place(x, y, to_z, to_core))

    def x_copy(layer, step):
        to = lax.rem(x + step, 4)
        src = zbuf.at[layer - 1, to]
        dst = out.at[layer, :, group_cols(x)]
        return remote(src, dst, xs.at[layer - 1, step - 1], xr.at[layer - 1, step - 1], place(to, y, z, core))

    def z_send(layer):
        y_wait(layer)
        for step, flip in zorder:
            z_copy(layer, step, flip).start()

    def x_send(layer):
        for step, flip in zorder:
            if step * 2 + flip == 0:
                z_copy(layer, 0, 0).wait()
            else:
                z_copy(layer, step, flip).wait_recv()
        for step in others:
            x_copy(layer, step).start()
        out[layer, :, group_cols(x)] = zbuf[layer - 1, x]

    barrier = pltpu.get_barrier_semaphore()
    peers = [place(x, lax.rem(y + step, 4), z, core) for step in others]
    peers += [place(lax.rem(x + step, 4), y, z, core) for step in others]
    peers += [place(x, y, lax.rem(z + step, 4), lax.rem(core + flip, 2)) for step, flip in zorder if step or flip]
    for peer_device in peers:
        pl.semaphore_signal(barrier, inc=1, device_id=peer_device, device_id_type=MESH)
    tables = [pltpu.make_async_copy(counts_hbm, counts, cs.at[0]), pltpu.make_async_copy(blocks_hbm, blocks, cs.at[1])]
    for copy in tables:
        copy.start()
    for u in range(ROUNDS):
        y_copy(0, 0, u).start()
    pl.semaphore_wait(barrier, len(peers))

    @pl.loop(0, ROUNDS)
    def _(u):
        for step in others:
            y_copy(0, step, u).start()

    @pl.loop(1, LAYERS)
    def _(layer):
        for step in others + (0,):
            y_copy(layer, step).start()

    def q_send(kv):
        for rel in (3, 2, 1, 0):
            q_copy(kv, rel).start()

    q_send(0)

    @pl.loop(0, ROUNDS + 1)
    def _(t):
        @pl.when(t < ROUNDS)
        def _():
            y_wait(0, t)
            z0_copy(t, 1).start()
            z0_copy(t, 0).start()

        @pl.when(t >= 1)
        def _():
            z0_copy(t - 1, 1).wait_recv()
            z0_copy(t - 1, 0).wait()
            for step in others:
                when_is(lax.rem(x + step, 4), range(4), lambda v: g_copy(t - 1, step, v + 1).start())

        when_is(t, (2,), lambda v: q_send(1))

    for copy in tables:
        copy.wait()
    slot = lax.broadcasted_iota(jnp.int32, (1, SEQD), 1)
    second = slot // SUMLEN
    for doc in range(8):
        at = doc * 8 + d
        live_blocks = jnp.where(second == 0, blocks[0, at], blocks[1, at])
        live = (second < counts[at]) & (slot - second * SUMLEN < BLOCK * live_blocks)
        bias[doc : doc + 1, :] = jnp.where(live, 0.0, NEGATIVE)

    @pl.loop(1, 5)
    def _(layer):
        z_send(layer)

    def gathered(v):
        @pl.loop(0, ROUNDS)
        def _(u):
            for step in others:
                g_copy(u, step, v + 1).wait_recv()

    when_is(x, range(4), gathered)
    x_send(1)

    @pl.loop(0, 8)
    def _(t):
        rel = 3 - t // 2
        kv = lax.rem(t, 2)
        to_zh, to_core = peer(rel)
        pltpu.make_async_copy(queries.at[:, group_cols(0)], qbuf.at[kv, 0], qr.at[kv, rel]).wait()
        src = to_zh * 2 + to_core
        for g in range(GROUP):
            qstack[g * 256 : (g + 1) * 256, :] = qbuf[kv, src, :, g * HD : (g + 1) * HD]
        result = head_group(
            x * 2 + to_zh, to_core, qstack, keys.at[kv], keys.at[2 + kv], bias, s_ref, m_ref, l_ref, acc_ref
        )
        for g in range(GROUP):
            obuf[kv, src, :, g * HD : (g + 1) * HD] = result[g * 256 : (g + 1) * 256]

        @pl.when((t == 0) | (t == 2) | (t == 3))
        def _():
            z_send(t - t // 2 + 5)
            x_send(t - t // 2 + 2)

        @pl.when((t == 4) | (t == 5))
        def _():
            x_send(t + 1)

        @pl.when(t == 3)
        def _():
            for rel in (3, 2):
                for kv in range(2):
                    o_copy(kv, rel).start()

        @pl.when((t == 4) | (t == 5))
        def _():
            o_copy(kv, 1).start()

        @pl.when(t >= 6)
        def _():
            attended[:, group_cols(kv * 4 + chunk)] = obuf[kv, chunk]

        @pl.when(t == 4)
        def _():
            for rel in (3, 2, 1):
                for frm in range(4):
                    l_copy(frm, rel).start()
            for frm in range(4):
                out[0, :, head_cols(frm * 4 + chunk)] = keys[frm, x, zh, half_rows(core)]

        @pl.when(t == 7)
        def _():
            x_send(7)

    @pl.loop(0, ROUNDS)
    def _(u):
        for step in others:
            y_copy(0, step, u).wait_send()
            when_is(lax.rem(x + step, 4), range(4), lambda v: g_copy(u, step, v + 1).wait_send())
        z0_copy(u, 1).wait_send()

    for kv in range(2):
        for rel in (1, 2, 3):
            q_copy(kv, rel).wait_send()

    @pl.loop(1, LAYERS)
    def _(layer):
        for step in others:
            y_copy(layer, step).wait_send()
        for step, flip in zorder:
            if step * 2 + flip:
                z_copy(layer, step, flip).wait_send()
        for step in others:
            x_copy(layer, step).wait()

    for kv in range(2):
        for rel in (1, 2, 3):
            o_copy(kv, rel).wait()

    for frm in range(4):
        for rel in (1, 2, 3):
            l_copy(frm, rel).wait()


def relay(cache, queries, counts, blocks):
    dma = pltpu.SemaphoreType.DMA
    bf = jnp.bfloat16
    f32 = jnp.float32
    rows = GROUP * 256
    anyspace = pl.BlockSpec(memory_space=pl.ANY)
    sems = [
        (4, 3), (4, 3), (4,), (7, 3), (7, 3), (7,), (4,), (4,), (4,), (7, 8), (7, 8), (4, 3), (4, 3),
        (7, 3), (7, 3), (4, 4), (4, 4), (2, 4), (2, 4), (2, 4), (2, 4), (2,),
    ]
    return pl.pallas_call(
        relay_kernel,
        out_shape=(
            jax.ShapeDtypeStruct((LAYERS, 256, 2048), bf),
            jax.ShapeDtypeStruct((256, QH * HD), bf),
            jax.ShapeDtypeStruct((LAYERS, 2, 2, 2, SEQD, HD), bf),
        ),
        in_specs=[anyspace] * 4,
        out_specs=(pl.BlockSpec(memory_space=pltpu.VMEM),) * 2 + (anyspace,),
        scratch_shapes=[
            pltpu.VMEM((8, SEQD), f32),
            pltpu.SMEM((64,), jnp.int32),
            pltpu.SMEM((SECTIONS, 64), jnp.int32),
            pltpu.VMEM((4, 4, 2, SEQD, HD), bf),
            pltpu.VMEM((LAYERS - 1, 4, 256, 4 * HD), bf),
            pltpu.VMEM((2, 4, 256, GROUP * HD), bf),
            pltpu.VMEM((2, 4, 256, GROUP * HD), bf),
            pltpu.VMEM((rows, HD), bf),
            pltpu.VMEM((8, rows, SEQD), f32),
            pltpu.VMEM((rows, 128), f32),
            pltpu.VMEM((rows, 128), f32),
            pltpu.VMEM((rows, HD), f32),
        ]
        + [dma(shape) for shape in sems],
        compiler_params=pltpu.CompilerParams(collective_id=0, has_side_effects=True, vmem_limit_bytes=40 << 20),
    )(cache.reshape(LAYERS, 2, 2, 2, SEQD, HD), *(pltpu.with_memory_space_constraint(a, pltpu.HBM) for a in (queries, counts, blocks.T)))


def settle_kernel(out, attended, out_to, attended_to, sems):
    copies = [pltpu.make_async_copy(out.at[layer], out_to.at[layer], sems.at[layer]) for layer in range(LAYERS)]
    copies.append(pltpu.make_async_copy(attended, attended_to, sems.at[LAYERS]))
    for copy in copies:
        copy.start()
    for copy in copies:
        copy.wait()


def settle(out, attended):
    vmem, anyspace = pl.BlockSpec(memory_space=pltpu.VMEM), pl.BlockSpec(memory_space=pl.ANY)
    return pl.pallas_call(
        settle_kernel,
        out_shape=tuple(jax.ShapeDtypeStruct(a.shape, a.dtype) for a in (out, attended)),
        in_specs=[vmem, vmem],
        out_specs=(anyspace, anyspace),
        scratch_shapes=[pltpu.SemaphoreType.DMA((LAYERS + 1,))],
        compiler_params=pltpu.CompilerParams(vmem_limit_bytes=16 << 20),
    )(out, attended)


def local(summary_cache, queries, section_counts, summary_blocks):
    relayed, attended, _ = relay(summary_cache, queries[0], section_counts, summary_blocks)
    relayed, attended = settle(relayed, attended)
    return attended[None], relayed[:, None]


def solution(mesh):
    placed = (P(None, "doc", None, "ctx"), P("doc", "ctx", None), P(), P())
    return jax.shard_map(
        local,
        mesh=mesh,
        in_specs=placed,
        out_specs=(P("doc", "ctx", None), P(None, "doc", "ctx", None)),
        check_vma=False,
    )
```
